512 devices in a mesh: ep: 128 (over x, z, core), dp: 4 (over y).
Axes of the slice: x: 4, y: 4, z: 16, core: 2. Of those that a mesh axis runs over, the one named last changes fastest.
Arguments:
- tokens: bfloat16 [2048, 3584], P('ep'), may hold values from -6 to 6
- expert_ids: int32 [2048, 8], P('ep'), may hold values from 0 to 127, all different within a row; in each aligned block of 16 rows (0 to 15, 16 to 31, ...) at most 4 rows name the same one
- route_logits: float32 [2048, 8], P('ep'), may hold values from -8 to 8
- expert_gate: bfloat16 [128, 3584, 1024], P('ep', None, 'dp'), may hold values from -0.09375 to 0.09375
- expert_up: bfloat16 [128, 3584, 1024], P('ep', None, 'dp'), may hold values from -0.09375 to 0.09375
- expert_down: bfloat16 [128, 1024, 3584], P('ep', 'dp'), may hold values from -0.1875 to 0.1875
Outputs:
- mixed: bfloat16 [2048, 3584], P(('ep', 'dp'))
The draws below stay inside these ranges and needn't reach their ends.
Inputs may be any that keep to these rules, and one draw needn't show every extreme that they name: `expert_ids`: each row names 8 different experts of 0 to 127 and every expert is named by some row. Within the rows of one index of ep (aligned blocks of 16 rows) no expert is named more than 4 times, and some block names one expert exactly 4 times. Loads are heavy-tailed: a few experts take several times the mean.
All inputs are finite; a program needn't handle non-finite values.
Results may differ from the reference program's by a relative error of at most 0.015.
Values may be sent and summed in bfloat16 or wider, within the bound.
No kernel may reach another device: no remote copies, remote signals or barrier semaphores. Data moves between devices by JAX's collectives and lax.ppermute only.
A program may use at most 64 MiB of HBM per device.

```python
import math
import jax
import jax.numpy as jnp
import numpy as np
from jax import lax

D = 3584
FF = 1024
TOP = 8
TOK_EP = 16
EXPERTS = 128
TOKENS = 2048
CAP = 4


def block_levels(own_key, shape, cuts, smallest, largest):
    gain = 1.0
    for position, parts in cuts:
        steps = jax.random.uniform(jax.random.fold_in(jax.random.fold_in(own_key, 6), position), (parts,), jnp.float32, smallest / len(cuts), largest / len(cuts))
        gain = gain * jnp.repeat(jnp.exp(steps), shape[position] // parts).reshape((-1,) + (1,) * (len(shape) - 1 - position))
    return gain


def deal_out(key, own, number, rows, amount, top, reach, lean):
    sequence = jax.random.permutation(key, amount)
    heavy_load, usual = load_shares(amount, rows * top, reach, lean, True), load_shares(amount, rows * top, reach, lean, False)
    places = jnp.arange(amount)

    def named(tallies, rotation):
        used = int((tallies > 0).sum())
        fixed = max(1, used // 4)
        shifted = fixed + (places - fixed + rotation * (used - fixed)) % max(1, amount - fixed)
        return jnp.zeros((amount,), jnp.int32).at[sequence[jnp.where(places < fixed, places, shifted)]].set(jnp.asarray(tallies, jnp.int32))

    tallies = jnp.where(number % 4 == 0, named(heavy_load, number // 4), named(usual, number - number // 4 - 1))
    mixed = jax.random.permutation(jax.random.fold_in(own, 3), amount)
    donor, taker = mixed[0:amount // 2 * 2:2], mixed[1:amount // 2 * 2:2]
    margin = jnp.minimum(tallies[donor] - 1, reach - tallies[taker]) // 2
    margin = jnp.where((donor == sequence[0]) | (taker == sequence[0]) | (tallies[taker] == 0), 0, jnp.maximum(margin, 0))
    shifted = jax.random.randint(jax.random.fold_in(own, 4), (amount // 2,), 0, 1 << 20) % (margin + 1)
    tallies = tallies.at[donor].add(-shifted).at[taker].add(shifted)
    members = jnp.searchsorted(jnp.cumsum(tallies), jnp.arange(rows * top), side="right").astype(jnp.int32)
    listing = members.reshape(top, rows).T
    listing = listing[jax.random.permutation(jax.random.fold_in(own, 1), rows)]
    rotation = jax.random.randint(jax.random.fold_in(own, 2), (rows, 1), 0, top)
    return jnp.take_along_axis(listing, (jnp.arange(top)[None, :] + rotation) % top, axis=1)


def load_shares(count, total, bound, slope, full):
    loads = [(1 << 20) // math.isqrt(standing ** slope) + 1 for standing in range(1, count + 1)]
    largest = bound if full else min(bound, max(-(-total // count), total * loads[0] // sum(loads)))
    least = 1 if total - largest >= count - 1 else 0
    given, spare = [largest] + [least] * (count - 1), total - largest - least * (count - 1)
    while spare > 0:
        free = [i for i in range(1, count) if given[i] < largest] or [i for i in range(1, count) if given[i] < bound]
        pool, remaining = sum([loads[i] for i in free]), spare
        for i in free:
            extra = min(bound - given[i], max(1, remaining * loads[i] // pool), spare)
            given[i] = given[i] + extra
            spare = spare - extra
    return np.array(given)


def scatter_about(rng, extent, scale, most, cuts=(), held_as=jnp.bfloat16):
    result = jax.random.normal(rng, extent, jnp.float32) * scale
    if len(cuts) > 0:
        result = block_levels(rng, extent, cuts, -0.22, 0.18) * result
    return jnp.clip(result, min=-most, max=most).astype(held_as)


def setup_inputs(seed: int = 0) -> dict:
    key_of = jax.random.split(jax.random.key(seed), 7)
    tokens = scatter_about(key_of[0], (TOKENS, D), 1.0, 6.0, ((0, 128),))
    expert_ids_keys = jax.random.split(jax.random.fold_in(key_of[1], 1), TOKENS // TOK_EP)
    expert_ids_turns = jax.random.permutation(jax.random.fold_in(key_of[1], 3), TOKENS // TOK_EP)
    expert_ids = jax.vmap(lambda own, number: deal_out(jax.random.fold_in(key_of[1], 2), own, number, TOK_EP, EXPERTS, TOP, CAP, 3))(expert_ids_keys, expert_ids_turns).reshape((TOKENS, TOP))
    route_logits = scatter_about(key_of[2], (TOKENS, TOP), 2.0, 8.0, ((0, 128),), jnp.float32)
    expert_gate = scatter_about(key_of[3], (EXPERTS, D, FF), D ** -0.5, 0.09375, ((0, 128), (2, 4)))
    expert_up = scatter_about(key_of[4], (EXPERTS, D, FF), D ** -0.5, 0.09375, ((0, 128), (2, 4)))
    expert_down = scatter_about(key_of[5], (EXPERTS, FF, D), FF ** -0.5, 0.1875, ((0, 128), (1, 4)))
    return dict(tokens=tokens, expert_ids=expert_ids, route_logits=route_logits, expert_gate=expert_gate, expert_up=expert_up, expert_down=expert_down)


route_scale = 2.5


def expert_rows(rows, w_gate, w_up, w_down):
    gate = jnp.dot(rows, w_gate, preferred_element_type=jnp.float32)
    upper = jnp.dot(rows, w_up, preferred_element_type=jnp.float32)
    hidden = (jax.nn.silu(gate) * upper).astype(jnp.bfloat16)
    return jnp.dot(hidden, w_down, preferred_element_type=jnp.float32).astype(jnp.bfloat16)


def reference(tokens, expert_ids, route_logits, expert_gate, expert_up, expert_down):
    token_count, width = tokens.shape
    top = expert_ids.shape[1]
    experts = expert_gate.shape[0]
    flat_ids = expert_ids.reshape(-1).astype(jnp.int32)
    slots = flat_ids.shape[0]
    block_rows = 64
    counts = jnp.zeros((experts,), jnp.int32).at[flat_ids].add(1).astype(jnp.int32)
    padded = (((counts + block_rows - 1) // block_rows) * block_rows).astype(jnp.int32)
    pad_start = (jnp.cumsum(padded) - padded).astype(jnp.int32)
    seg_start = (jnp.cumsum(counts) - counts).astype(jnp.int32)
    sorted_slots = jnp.argsort(flat_ids, stable=True).astype(jnp.int32)
    sorted_ids = flat_ids[sorted_slots]
    within = (jnp.arange(slots, dtype=jnp.int32) - seg_start[sorted_ids]).astype(jnp.int32)
    target = (pad_start[sorted_ids] + within).astype(jnp.int32)
    nblocks = (slots + experts * (block_rows - 1)) // block_rows + 1
    row_token = jnp.full((nblocks * block_rows,), token_count, jnp.int32).at[target].set((sorted_slots // top).astype(jnp.int32))
    pad_end = pad_start + padded
    block_start = jnp.arange(nblocks, dtype=jnp.int32) * block_rows
    block_expert = jnp.sum((pad_end[None, :] <= block_start[:, None]).astype(jnp.int32), axis=1)
    block_expert = jnp.minimum(block_expert, experts - 1).astype(jnp.int32)
    extended = jnp.concatenate([tokens, jnp.zeros((1, width), tokens.dtype)], axis=0)

    def one_block(inputs):
        block_index, expert = inputs
        picks = lax.dynamic_slice_in_dim(row_token, (block_index * block_rows).astype(jnp.int32), block_rows, 0)
        return expert_rows(extended[picks], expert_gate[expert], expert_up[expert], expert_down[expert])

    outputs = lax.map(one_block, (jnp.arange(nblocks, dtype=jnp.int32), block_expert))
    outputs = outputs.reshape(nblocks * block_rows, width)
    slot_target = jnp.zeros((slots,), jnp.int32).at[sorted_slots].set(target)
    slot_values = outputs[slot_target].reshape(token_count, top, width)
    scores = jax.nn.sigmoid(route_logits)
    weights = route_scale * scores / jnp.sum(scores, axis=1, keepdims=True)
    routed = jnp.sum(weights[:, :, None] * slot_values.astype(jnp.float32), axis=1)
    return routed.astype(jnp.bfloat16)
```

```python
import jax
import jax.numpy as jnp
from jax import lax
from jax.experimental import pallas as pl
from jax.experimental.pallas import tpu as pltpu
from jax.sharding import Mesh, PartitionSpec as P


route_scale = 2.5
SIDE = 128
SLOTS = 4
CHIPS_X, CORES = 4, 2

f32, bf16, i32 = jnp.float32, jnp.bfloat16, jnp.int32
VMEM = pl.BlockSpec(memory_space=pltpu.VMEM)
SMEM = pl.BlockSpec(memory_space=pltpu.SMEM)


def pack_rows(tokens, expert_ids, route_logits, member, n_dp):
    rows, width = tokens.shape
    top = expert_ids.shape[1]
    part = width // n_dp

    def body(member_ref, tokens_ref, ids_ref, logits_ref, out_ref):
        start = pl.multiple_of(member_ref[0] * part, 128)
        out_ref[:, :part] = tokens_ref[:, pl.ds(start, part)]
        scores = 1.0 / (1.0 + jnp.exp(-logits_ref[...]))
        weights = route_scale * scores / jnp.sum(scores, axis=0, keepdims=True)
        high = weights.astype(bf16).astype(f32)
        side = jnp.concatenate(
            [ids_ref[...].astype(f32), high, weights - high, jnp.zeros((SIDE - 3 * top, rows), f32)], axis=0
        )
        out_ref[:, part:] = side.T.astype(bf16)

    return pl.pallas_call(
        body,
        out_shape=jax.ShapeDtypeStruct((rows, part + SIDE), bf16),
        in_specs=[SMEM, VMEM, VMEM, VMEM],
        out_specs=VMEM,
        name="pack_rows",
    )(member, tokens, expert_ids.T, route_logits.T)


def route_rows(gathered, plane, rows, top, n_x, n_z, n_c, n_dp):
    total = gathered.shape[0]
    part = gathered.shape[1] - SIDE
    experts = n_x * n_c
    held = n_z * SLOTS
    pad = max(16, experts)

    def body(plane_ref, gathered_ref, out_ref, high_ref, low_ref, pick_ref):
        side = gathered_ref[:, part:].astype(f32).T
        line = lax.broadcasted_iota(i32, (pad, 1), 0)
        name = ((line // n_c) * n_z + plane_ref[0]) * n_c + line % n_c
        name = jnp.where(line < experts, name, -1).astype(f32)
        named = jnp.zeros((pad, total), f32)
        high = jnp.zeros((pad, total), f32)
        low = jnp.zeros((pad, total), f32)
        for k in range(top):
            same = side[k : k + 1, :] == name
            named = named + jnp.where(same, 1.0, 0.0)
            high = high + jnp.where(same, side[top + k : top + k + 1, :], 0.0)
            low = low + jnp.where(same, side[2 * top + k : 2 * top + k + 1, :], 0.0)
        one = lax.broadcasted_iota(i32, (total, total), 0)
        two = lax.broadcasted_iota(i32, (total, total), 1)
        ahead = jnp.where((one // rows == two // rows) & (one < two), 1.0, 0.0).astype(bf16)
        rank = jnp.dot(named.astype(bf16), ahead, preferred_element_type=f32)
        rank = jnp.where(named > 0.5, rank, -1.0)
        spot = lax.broadcasted_iota(i32, (held, total), 0)
        token = lax.broadcasted_iota(i32, (held, total), 1)
        wanted = jnp.where(token // rows == spot // SLOTS, spot % SLOTS, -2).astype(f32)
        for j in range(experts):
            hit = rank[j : j + 1, :] == wanted
            at = slice(j * held, (j + 1) * held)
            pick_ref[at, :] = jnp.where(hit, 1.0, 0.0).astype(bf16)
            high_ref[at, :] = jnp.where(hit, high[j : j + 1, :], 0.0).astype(bf16)
            low_ref[at, :] = jnp.where(hit, low[j : j + 1, :], 0.0).astype(bf16)
        sent = jnp.dot(pick_ref[...], gathered_ref[:, :part], preferred_element_type=f32).astype(bf16)
        for d in range(n_dp):
            out_ref[d] = sent

    slots = experts * held
    return pl.pallas_call(
        body,
        out_shape=(
            jax.ShapeDtypeStruct((n_dp, slots, part), bf16),
            jax.ShapeDtypeStruct((slots, total), bf16),
            jax.ShapeDtypeStruct((slots, total), bf16),
        ),
        in_specs=[SMEM, VMEM],
        out_specs=(VMEM, VMEM, VMEM),
        scratch_shapes=[pltpu.VMEM((slots, total), bf16)],
        name="route_rows",
    )(plane, gathered)


def hidden_rows(received, w_gate, w_up):
    n_dp, slots, part = received.shape
    units = w_gate.shape[1]

    def body(rows_ref, gate_ref, up_ref, out_ref, sum_gate, sum_up):
        step = pl.program_id(0)

        @pl.when(step == 0)
        def _():
            sum_gate[...] = jnp.zeros_like(sum_gate)
            sum_up[...] = jnp.zeros_like(sum_up)

        rows = rows_ref[0]
        sum_gate[...] += jnp.dot(rows, gate_ref[...], preferred_element_type=f32)
        sum_up[...] += jnp.dot(rows, up_ref[...], preferred_element_type=f32)

        @pl.when(step == n_dp - 1)
        def _():
            v = sum_gate[...]
            made = (v / (1.0 + jnp.exp(-v)) * sum_up[...]).astype(bf16)
            for d in range(n_dp):
                out_ref[d] = made

    return pl.pallas_call(
        body,
        grid=(n_dp,),
        out_shape=jax.ShapeDtypeStruct((n_dp, slots, units), bf16),
        in_specs=[
            pl.BlockSpec((1, slots, part), lambda i: (i, 0, 0)),
            pl.BlockSpec((part, units), lambda i: (i, 0)),
            pl.BlockSpec((part, units), lambda i: (i, 0)),
        ],
        out_specs=pl.BlockSpec((n_dp, slots, units), lambda i: (0, 0, 0)),
        scratch_shapes=[pltpu.VMEM((slots, units), f32), pltpu.VMEM((slots, units), f32)],
        name="hidden_rows",
    )(received, w_gate, w_up)


def output_rows(hidden, downs, member):
    n_dp, slots, _ = hidden.shape
    _, part = downs[0].shape

    def body(member_ref, hidden_ref, *refs):
        out_ref = refs[-1]
        total = jnp.zeros((slots, part), f32)
        for s in range(n_dp):
            source = lax.rem(member_ref[0] + (n_dp - s), n_dp)
            total = total + jnp.dot(hidden_ref[source], refs[s][...], preferred_element_type=f32)
        out_ref[...] = total.astype(bf16)

    return pl.pallas_call(
        body,
        out_shape=jax.ShapeDtypeStruct((slots, part), bf16),
        in_specs=[SMEM, VMEM] + [VMEM] * n_dp,
        out_specs=VMEM,
        name="output_rows",
    )(member, hidden, *downs)


def mix_rows(received, high, low):
    _, part = received.shape
    total = high.shape[1]

    def body(rows_ref, high_ref, low_ref, out_ref):
        rows = rows_ref[...]
        dims = (((0,), (0,)), ((), ()))
        mixed = lax.dot_general(high_ref[...], rows, dims, preferred_element_type=f32)
        mixed = mixed + lax.dot_general(low_ref[...], rows, dims, preferred_element_type=f32)
        out_ref[...] = mixed.astype(bf16)

    return pl.pallas_call(
        body,
        out_shape=jax.ShapeDtypeStruct((total, part), bf16),
        in_specs=[VMEM, VMEM, VMEM],
        out_specs=VMEM,
        name="mix_rows",
    )(received, high, low)


def sum_rows(shares):
    n_z, rows, part = shares.shape

    def body(shares_ref, out_ref):
        total = shares_ref[0].astype(f32)
        for z in range(1, n_z):
            total = total + shares_ref[z].astype(f32)
        out_ref[...] = total.astype(bf16)

    return pl.pallas_call(
        body,
        out_shape=jax.ShapeDtypeStruct((rows, part), bf16),
        in_specs=[VMEM],
        out_specs=VMEM,
        name="sum_rows",
    )(shares)


def on_device(tokens, expert_ids, route_logits, expert_gate, expert_up, expert_down):
    rows, width = tokens.shape
    top = expert_ids.shape[1]
    n_x, n_z, n_c, n_dp = (lax.axis_size(a) for a in ("x", "z", "c", "y"))
    part = width // n_dp
    held = n_z * SLOTS
    slots = n_x * n_c * held
    member = lax.axis_index("y").astype(i32)
    member_ref = member.reshape(1)
    plane_ref = lax.axis_index("z").astype(i32).reshape(1)

    downs = []
    for s in range(n_dp):
        owner = member + s
        owner = jnp.where(owner >= n_dp, owner - n_dp, owner)
        piece = lax.dynamic_slice_in_dim(expert_down[0], owner * part, part, axis=1)
        if s:
            piece = lax.ppermute(piece, "y", [(i, (i + s) % n_dp) for i in range(n_dp)])
        downs.append(piece)

    packed = pack_rows(tokens, expert_ids, route_logits, member_ref, n_dp)
    gathered = lax.all_gather(packed, "z", axis=0, tiled=True)
    outgoing, high, low = route_rows(gathered, plane_ref, rows, top, n_x, n_z, n_c, n_dp)
    outgoing = outgoing.reshape(n_dp * n_x * n_c, held, part)
    arrived = lax.all_to_all(outgoing, ("y", "x", "c"), split_axis=0, concat_axis=0, tiled=True)
    hidden = hidden_rows(arrived.reshape(n_dp, slots, part), expert_gate[0], expert_up[0])
    hidden = lax.all_to_all(hidden, "y", split_axis=0, concat_axis=0, tiled=True)
    results = output_rows(hidden, downs, member_ref)
    results = results.reshape(n_x * n_c, held, part)
    back = lax.all_to_all(results, ("x", "c"), split_axis=0, concat_axis=0, tiled=True)
    mixed = mix_rows(back.reshape(slots, part), high, low)
    mixed = mixed.reshape(n_z, rows, part)
    shares = lax.all_to_all(mixed, "z", split_axis=0, concat_axis=0, tiled=True)
    routed = sum_rows(shares)
    return lax.all_to_all(routed, "y", split_axis=0, concat_axis=1, tiled=True)


def solution(mesh):
    n_ep, n_dp = mesh.devices.shape
    grid = mesh.devices.reshape(CHIPS_X, n_ep // (CHIPS_X * CORES), CORES, n_dp)
    fine = Mesh(grid, ("x", "z", "c", "y"))
    ep = ("x", "z", "c")
    placed = (
        P(ep, None),
        P(ep, None),
        P(ep, None),
        P(ep, None, "y"),
        P(ep, None, "y"),
        P(ep, "y", None),
    )
    return jax.shard_map(
        on_device, mesh=fine, in_specs=placed, out_specs=P(ep + ("y",), None), check_vma=False
    )
```

```python
import jax
import jax.numpy as jnp
from jax import lax
from jax.experimental import pallas as pl
from jax.experimental.pallas import tpu as pltpu
from jax.sharding import Mesh, PartitionSpec as P


route_scale = 2.5
SIDE = 128
SLOTS = 4
CHIPS_X, CORES = 4, 2

f32, bf16, i32 = jnp.float32, jnp.bfloat16, jnp.int32
PARAMS = pltpu.CompilerParams(vmem_limit_bytes=20 * 1024 * 1024)
VMEM = pl.BlockSpec(memory_space=pltpu.VMEM)
SMEM = pl.BlockSpec(memory_space=pltpu.SMEM)


def call(body, outs, ins, scratch=()):
    many = isinstance(outs, tuple)
    return pl.pallas_call(
        body,
        out_shape=tuple(jax.ShapeDtypeStruct(*o) for o in outs) if many else jax.ShapeDtypeStruct(*outs[0]),
        in_specs=ins,
        out_specs=(VMEM,) * len(outs) if many else VMEM,
        scratch_shapes=list(scratch),
        compiler_params=PARAMS,
    )


def pack_rows(tokens, expert_ids, route_logits, member, n_dp, n_z):
    rows, width = tokens.shape
    top = expert_ids.shape[1]
    part = width // n_dp

    def body(member_ref, tokens_ref, ids_ref, logits_ref, out_ref):
        start = pl.multiple_of(member_ref[0] * part, 128)
        own = tokens_ref[:, pl.ds(start, part)]
        scores = 1.0 / (1.0 + jnp.exp(-logits_ref[...]))
        weights = route_scale * scores / jnp.sum(scores, axis=0, keepdims=True)
        high = weights.astype(bf16).astype(f32)
        side = jnp.concatenate(
            [ids_ref[...].astype(f32), high, weights - high, jnp.zeros((SIDE - 3 * top, rows), f32)], axis=0
        )
        side = side.T.astype(bf16)
        for z in range(n_z):
            out_ref[z, :, :part] = own
            out_ref[z, :, part:] = side

    outs = [((n_z, rows, part + SIDE), bf16)]
    return call(body, outs, [SMEM, VMEM, VMEM, VMEM])(member, tokens, expert_ids.T, route_logits.T)


def route_rows(gathered, plane, rows, top, n_x, n_z, n_c, n_dp):
    total = gathered.shape[0]
    part = gathered.shape[1] - SIDE
    experts = n_x * n_c
    held = n_z * SLOTS
    pad = max(16, experts)

    def body(plane_ref, gathered_ref, out_ref, high_ref, low_ref, pick_ref):
        side = gathered_ref[:, part:].astype(f32).T
        line = lax.broadcasted_iota(i32, (pad, 1), 0)
        name = ((line // n_c) * n_z + plane_ref[0]) * n_c + line % n_c
        name = jnp.where(line < experts, name, -1).astype(f32)
        named = jnp.zeros((pad, total), f32)
        high = jnp.zeros((pad, total), f32)
        low = jnp.zeros((pad, total), f32)
        for k in range(top):
            same = side[k : k + 1, :] == name
            named = named + jnp.where(same, 1.0, 0.0)
            high = high + jnp.where(same, side[top + k : top + k + 1, :], 0.0)
            low = low + jnp.where(same, side[2 * top + k : 2 * top + k + 1, :], 0.0)
        one = lax.broadcasted_iota(i32, (total, total), 0)
        two = lax.broadcasted_iota(i32, (total, total), 1)
        ahead = jnp.where((one // rows == two // rows) & (one < two), 1.0, 0.0).astype(bf16)
        rank = jnp.dot(named.astype(bf16), ahead, preferred_element_type=f32)
        rank = jnp.where(named > 0.5, rank, -1.0)
        spot = lax.broadcasted_iota(i32, (held, total), 0)
        token = lax.broadcasted_iota(i32, (held, total), 1)
        wanted = jnp.where(token // rows == spot // SLOTS, spot % SLOTS, -2).astype(f32)
        for j in range(experts):
            hit = rank[j : j + 1, :] == wanted
            at = slice(j * held, (j + 1) * held)
            pick_ref[at, :] = jnp.where(hit, 1.0, 0.0).astype(bf16)
            high_ref[at, :] = jnp.where(hit, high[j : j + 1, :], 0.0).astype(bf16)
            low_ref[at, :] = jnp.where(hit, low[j : j + 1, :], 0.0).astype(bf16)
        sent = jnp.dot(pick_ref[...], gathered_ref[:, :part], preferred_element_type=f32).astype(bf16)
        for d in range(n_dp):
            out_ref[d] = sent

    slots = experts * held
    outs = (((n_dp, slots, part), bf16),) + (((slots, total), bf16),) * 2
    scratch = [pltpu.VMEM((slots, total), bf16)]
    return call(body, outs, [SMEM, VMEM], scratch)(plane, gathered)


def hidden_rows(received, w_gate, w_up):
    n_dp, slots, part = received.shape
    units = w_gate.shape[1]

    def body(rows_ref, gate_ref, up_ref, out_ref, sum_gate, sum_up):
        step = pl.program_id(0)

        @pl.when(step == 0)
        def _():
            sum_gate[...] = jnp.zeros_like(sum_gate)
            sum_up[...] = jnp.zeros_like(sum_up)

        rows = rows_ref[0]
        sum_gate[...] += jnp.dot(rows, gate_ref[...], preferred_element_type=f32)
        sum_up[...] += jnp.dot(rows, up_ref[...], preferred_element_type=f32)

        @pl.when(step == n_dp - 1)
        def _():
            v = sum_gate[...]
            made = (v / (1.0 + jnp.exp(-v)) * sum_up[...]).astype(bf16)
            for d in range(n_dp):
                out_ref[d] = made

    return pl.pallas_call(
        body,
        grid=(n_dp,),
        out_shape=jax.ShapeDtypeStruct((n_dp, slots, units), bf16),
        in_specs=[
            pl.BlockSpec((1, slots, part), lambda i: (i, 0, 0)),
            pl.BlockSpec((part, units), lambda i: (i, 0)),
            pl.BlockSpec((part, units), lambda i: (i, 0)),
        ],
        out_specs=pl.BlockSpec((n_dp, slots, units), lambda i: (0, 0, 0)),
        scratch_shapes=[pltpu.VMEM((slots, units), f32), pltpu.VMEM((slots, units), f32)],
        compiler_params=PARAMS,
        name="hidden_rows",
    )(received, w_gate, w_up)


def output_rows(hidden, downs, member):
    n_dp, slots, _ = hidden.shape
    part = downs[0].shape[1]

    def body(member_ref, hidden_ref, *refs):
        out_ref = refs[-1]
        total = jnp.zeros((slots, part), f32)
        for s in range(n_dp):
            source = lax.rem(member_ref[0] + (n_dp - s), n_dp)
            total = total + jnp.dot(hidden_ref[source], refs[s][...], preferred_element_type=f32)
        out_ref[...] = total.astype(bf16)

    return call(body, [((slots, part), bf16)], [SMEM, VMEM] + [VMEM] * n_dp)(
        member, hidden, *downs
    )


def mix_rows(received, high, low):
    _, part = received.shape
    total = high.shape[1]

    def body(rows_ref, high_ref, low_ref, out_ref):
        rows = rows_ref[...]
        dims = (((0,), (0,)), ((), ()))
        mixed = lax.dot_general(high_ref[...], rows, dims, preferred_element_type=f32)
        mixed = mixed + lax.dot_general(low_ref[...], rows, dims, preferred_element_type=f32)
        out_ref[...] = mixed.astype(bf16)

    return call(body, [((total, part), bf16)], [VMEM] * 3)(received, high, low)


def sum_rows(shares):
    n_z, rows, part = shares.shape

    def body(shares_ref, out_ref):
        total = shares_ref[0].astype(f32)
        for z in range(1, n_z):
            total = total + shares_ref[z].astype(f32)
        out_ref[...] = total.astype(bf16)

    return call(body, [((rows, part), bf16)], [VMEM])(shares)


def exchange(value, axes):
    return lax.all_to_all(value, axes, split_axis=0, concat_axis=0, tiled=True)


def on_device(tokens, expert_ids, route_logits, expert_gate, expert_up, expert_down):
    rows, width = tokens.shape
    top = expert_ids.shape[1]
    n_x, n_z, n_c, n_dp = (lax.axis_size(a) for a in ("x", "z", "c", "y"))
    part = width // n_dp
    held = n_z * SLOTS
    slots = n_x * n_c * held
    total = n_z * rows
    member = lax.axis_index("y").astype(i32)
    member_ref = member.reshape(1)
    plane_ref = lax.axis_index("z").astype(i32).reshape(1)
    w_gate, w_up = expert_gate[0], expert_up[0]

    packed = pack_rows(tokens, expert_ids, route_logits, member_ref, n_dp, n_z)
    gathered = exchange(packed, "z")

    downs = []
    for s in range(n_dp):
        owner = member + s
        owner = jnp.where(owner >= n_dp, owner - n_dp, owner)
        piece = lax.dynamic_slice_in_dim(expert_down[0], owner * part, part, axis=1)
        if s:
            piece = lax.ppermute(piece, "y", [(i, (i + s) % n_dp) for i in range(n_dp)])
        downs.append(piece)

    outgoing, high, low = route_rows(
        gathered.reshape(total, -1), plane_ref, rows, top, n_x, n_z, n_c, n_dp
    )
    arrived = exchange(outgoing.reshape(n_dp * n_x * n_c, held, part), ("y", "x", "c"))
    hidden = hidden_rows(arrived.reshape(n_dp, slots, part), w_gate, w_up)
    hidden = exchange(hidden, "y")
    results = output_rows(hidden, downs, member_ref)
    back = exchange(results.reshape(n_x * n_c, held, part), ("x", "c"))
    mixed = mix_rows(back.reshape(slots, part), high, low)
    shares = exchange(mixed.reshape(n_z, rows, part), "z")
    routed = sum_rows(shares)
    return lax.all_to_all(routed, "y", split_axis=0, concat_axis=1, tiled=True)


def solution(mesh):
    n_ep, n_dp = mesh.devices.shape
    grid = mesh.devices.reshape(CHIPS_X, n_ep // (CHIPS_X * CORES), CORES, n_dp)
    fine = Mesh(grid, ("x", "z", "c", "y"))
    ep = ("x", "z", "c")
    placed = (
        P(ep, None),
        P(ep, None),
        P(ep, None),
        P(ep, None, "y"),
        P(ep, None, "y"),
        P(ep, "y", None),
    )
    return jax.shard_map(
        on_device, mesh=fine, in_specs=placed, out_specs=P(ep + ("y",), None), check_vma=False
    )
```

```python
import jax
import jax.numpy as jnp
from jax import lax
from jax.experimental import pallas as pl
from jax.experimental.pallas import tpu as pltpu
from jax.sharding import Mesh, PartitionSpec as P


route_scale = 2.5
SIDE = 128
SLOTS = 4
CHIPS_X, CORES = 4, 2

f32, bf16, i32 = jnp.float32, jnp.bfloat16, jnp.int32
PARAMS = pltpu.CompilerParams(vmem_limit_bytes=20 * 1024 * 1024)
VMEM = pl.BlockSpec(memory_space=pltpu.VMEM)
HBM = pl.BlockSpec(memory_space=pltpu.HBM)
SMEM = pl.BlockSpec(memory_space=pltpu.SMEM)


def call(body, outs, ins, scratch=(), params=PARAMS):
    many = isinstance(outs, tuple)
    return pl.pallas_call(
        body,
        out_shape=tuple(jax.ShapeDtypeStruct(*o) for o in outs) if many else jax.ShapeDtypeStruct(*outs[0]),
        in_specs=ins,
        out_specs=(VMEM,) * len(outs) if many else VMEM,
        scratch_shapes=list(scratch),
        compiler_params=params,
    )


def pack_rows(tokens, expert_ids, route_logits, member, n_dp, n_z):
    rows, width = tokens.shape
    top = expert_ids.shape[1]
    part = width // n_dp

    def body(member_ref, tokens_hbm, ids_hbm, logits_hbm, out_ref, own_ref, ids_ref, logits_ref, sems):
        start = pl.multiple_of(member_ref[0] * part, 128)
        copies = [
            pltpu.make_async_copy(tokens_hbm.at[:, pl.ds(start, part)], own_ref, sems.at[0]),
            pltpu.make_async_copy(ids_hbm, ids_ref, sems.at[1]),
            pltpu.make_async_copy(logits_hbm, logits_ref, sems.at[2]),
        ]
        for copy in copies:
            copy.start()
        for copy in copies:
            copy.wait()
        own = own_ref[...]
        scores = 1.0 / (1.0 + jnp.exp(-logits_ref[...]))
        weights = route_scale * scores / jnp.sum(scores, axis=0, keepdims=True)
        high = weights.astype(bf16).astype(f32)
        side = jnp.concatenate(
            [ids_ref[...].astype(f32), high, weights - high, jnp.zeros((SIDE - 3 * top, rows), f32)], axis=0
        )
        side = side.T.astype(bf16)
        for z in range(n_z):
            out_ref[z, :, :part] = own
            out_ref[z, :, part:] = side

    outs = [((n_z, rows, part + SIDE), bf16)]
    scratch = [
        pltpu.VMEM((rows, part), bf16),
        pltpu.VMEM((top, rows), i32),
        pltpu.VMEM((top, rows), f32),
        pltpu.SemaphoreType.DMA((3,)),
    ]
    return call(body, outs, [SMEM, HBM, HBM, HBM], scratch, None)(member, tokens, expert_ids.T, route_logits.T)


def route_rows(gathered, plane, rows, top, n_x, n_z, n_c, n_dp):
    total = gathered.shape[0]
    part = gathered.shape[1] - SIDE
    experts = n_x * n_c
    held = n_z * SLOTS
    pad = max(16, experts)

    def body(plane_ref, gathered_ref, out_ref, high_ref, low_ref, pick_ref):
        side = gathered_ref[:, part:].astype(f32).T
        line = lax.broadcasted_iota(i32, (pad, 1), 0)
        name = ((line // n_c) * n_z + plane_ref[0]) * n_c + line % n_c
        name = jnp.where(line < experts, name, -1).astype(f32)
        named = jnp.zeros((pad, total), f32)
        high = jnp.zeros((pad, total), f32)
        low = jnp.zeros((pad, total), f32)
        for k in range(top):
            same = side[k : k + 1, :] == name
            named = named + jnp.where(same, 1.0, 0.0)
            high = high + jnp.where(same, side[top + k : top + k + 1, :], 0.0)
            low = low + jnp.where(same, side[2 * top + k : 2 * top + k + 1, :], 0.0)
        one = lax.broadcasted_iota(i32, (total, total), 0)
        two = lax.broadcasted_iota(i32, (total, total), 1)
        ahead = jnp.where((one // rows == two // rows) & (one < two), 1.0, 0.0).astype(bf16)
        rank = jnp.dot(named.astype(bf16), ahead, preferred_element_type=f32)
        rank = jnp.where(named > 0.5, rank, -1.0)
        spot = lax.broadcasted_iota(i32, (held, total), 0)
        token = lax.broadcasted_iota(i32, (held, total), 1)
        wanted = jnp.where(token // rows == spot // SLOTS, spot % SLOTS, -2).astype(f32)
        for j in range(experts):
            hit = rank[j : j + 1, :] == wanted
            at = slice(j * held, (j + 1) * held)
            pick_ref[at, :] = jnp.where(hit, 1.0, 0.0).astype(bf16)
            high_ref[at, :] = jnp.where(hit, high[j : j + 1, :], 0.0).astype(bf16)
            low_ref[at, :] = jnp.where(hit, low[j : j + 1, :], 0.0).astype(bf16)
        sent = jnp.dot(pick_ref[...], gathered_ref[:, :part], preferred_element_type=f32).astype(bf16)
        for d in range(n_dp):
            out_ref[d] = sent

    slots = experts * held
    outs = (((n_dp, slots, part), bf16),) + (((slots, total), bf16),) * 2
    scratch = [pltpu.VMEM((slots, total), bf16)]
    return call(body, outs, [SMEM, VMEM], scratch)(plane, gathered)


def hidden_rows(received, w_gate, w_up):
    n_dp, slots, part = received.shape
    units = w_gate.shape[1]

    def body(rows_ref, gate_ref, up_ref, out_ref):
        v = jnp.zeros((slots, units), f32)
        u = jnp.zeros((slots, units), f32)
        for d in range(n_dp):
            rows = rows_ref[d]
            at = slice(d * part, (d + 1) * part)
            v = v + jnp.dot(rows, gate_ref[at, :], preferred_element_type=f32)
            u = u + jnp.dot(rows, up_ref[at, :], preferred_element_type=f32)
        made = (v / (1.0 + jnp.exp(-v)) * u).astype(bf16)
        for d in range(n_dp):
            out_ref[d] = made

    return call(body, [((n_dp, slots, units), bf16)], [VMEM] * 3)(received, w_gate, w_up)


def output_rows(hidden, downs, member):
    n_dp, slots, _ = hidden.shape
    part = downs[0].shape[1]

    def body(member_ref, hidden_ref, *refs):
        out_ref = refs[-1]
        total = jnp.zeros((slots, part), f32)
        for s in range(n_dp):
            source = lax.rem(member_ref[0] + (n_dp - s), n_dp)
            total = total + jnp.dot(hidden_ref[source], refs[s][...], preferred_element_type=f32)
        out_ref[...] = total.astype(bf16)

    return call(body, [((slots, part), bf16)], [SMEM, VMEM] + [VMEM] * n_dp)(
        member, hidden, *downs
    )


def mix_rows(received, high, low, share):
    _, part = received.shape
    total = high.shape[1]

    def body(rows_ref, high_ref, low_ref, out_ref):
        rows = rows_ref[...]
        dims = (((0,), (0,)), ((), ()))
        mixed = lax.dot_general(high_ref[...], rows, dims, preferred_element_type=f32)
        mixed = mixed + lax.dot_general(low_ref[...], rows, dims, preferred_element_type=f32)
        for i in range(total // share):
            out_ref[i] = mixed[i * share : (i + 1) * share, :].astype(bf16)

    return call(body, [((total // share, share, part), bf16)], [VMEM] * 3)(received, high, low)


def sum_rows(shares, n_dp):
    peers, share, part = shares.shape

    def body(shares_ref, out_ref):
        for d in range(n_dp):
            total = shares_ref[d].astype(f32)
            for z in range(1, peers // n_dp):
                total = total + shares_ref[z * n_dp + d].astype(f32)
            out_ref[:, d * part : (d + 1) * part] = total.astype(bf16)

    return call(body, [((share, n_dp * part), bf16)], [VMEM])(shares)


def exchange(value, axes):
    return lax.all_to_all(value, axes, split_axis=0, concat_axis=0, tiled=True)


def on_device(tokens, expert_ids, route_logits, expert_gate, expert_up, expert_down):
    rows, width = tokens.shape
    top = expert_ids.shape[1]
    n_x, n_z, n_c, n_dp = (lax.axis_size(a) for a in ("x", "z", "c", "y"))
    part = width // n_dp
    held = n_z * SLOTS
    slots = n_x * n_c * held
    total = n_z * rows
    member = lax.axis_index("y").astype(i32)
    member_ref = member.reshape(1)
    plane_ref = lax.axis_index("z").astype(i32).reshape(1)
    w_gate, w_up = expert_gate[0], expert_up[0]

    packed = pack_rows(tokens, expert_ids, route_logits, member_ref, n_dp, n_z)
    gathered = exchange(packed, "z")

    downs = []
    for s in range(n_dp):
        owner = member + s
        owner = jnp.where(owner >= n_dp, owner - n_dp, owner)
        piece = lax.dynamic_slice_in_dim(expert_down[0], owner * part, part, axis=1)
        if s:
            piece = lax.ppermute(piece, "y", [(i, (i + s) % n_dp) for i in range(n_dp)])
        downs.append(piece)

    outgoing, high, low = route_rows(
        gathered.reshape(total, -1), plane_ref, rows, top, n_x, n_z, n_c, n_dp
    )
    arrived = exchange(outgoing.reshape(n_dp * n_x * n_c, held, part), ("y", "x", "c"))
    hidden = hidden_rows(arrived.reshape(n_dp, slots, part), w_gate, w_up)
    hidden, downs = lax.optimization_barrier((hidden, downs))
    hidden = exchange(hidden, "y")
    results = output_rows(hidden, downs, member_ref)
    back = exchange(results.reshape(n_x * n_c, held, part), ("x", "c"))
    mixed = mix_rows(back.reshape(slots, part), high, low, rows // n_dp)
    shares = exchange(mixed, ("z", "y"))
    return sum_rows(shares, n_dp)


def solution(mesh):
    n_ep, n_dp = mesh.devices.shape
    grid = mesh.devices.reshape(CHIPS_X, n_ep // (CHIPS_X * CORES), CORES, n_dp)
    fine = Mesh(grid, ("x", "z", "c", "y"))
    ep = ("x", "z", "c")
    placed = (
        P(ep, None),
        P(ep, None),
        P(ep, None),
        P(ep, None, "y"),
        P(ep, None, "y"),
        P(ep, "y", None),
    )
    return jax.shard_map(
        on_device, mesh=fine, in_specs=placed, out_specs=P(ep + ("y",), None), check_vma=False
    )
```

```python
import jax
import jax.numpy as jnp
from jax import lax
from jax.experimental import pallas as pl
from jax.experimental.pallas import tpu as pltpu
from jax.sharding import Mesh, PartitionSpec as P


route_scale = 2.5
SIDE = 128
SLOTS = 4
CHIPS_X, CORES = 4, 2

f32, bf16, i32 = jnp.float32, jnp.bfloat16, jnp.int32
PARAMS = pltpu.CompilerParams(vmem_limit_bytes=20 * 1024 * 1024)
VMEM = pl.BlockSpec(memory_space=pltpu.VMEM)
HBM = pl.BlockSpec(memory_space=pltpu.HBM)
SMEM = pl.BlockSpec(memory_space=pltpu.SMEM)


def call(body, outs, ins, scratch=(), params=PARAMS):
    many = isinstance(outs, tuple)
    return pl.pallas_call(
        body,
        out_shape=tuple(jax.ShapeDtypeStruct(*o) for o in outs) if many else jax.ShapeDtypeStruct(*outs[0]),
        in_specs=ins,
        out_specs=(VMEM,) * len(outs) if many else VMEM,
        scratch_shapes=list(scratch),
        compiler_params=params,
    )


def pack_rows(tokens, expert_ids, route_logits, member, n_dp, peers):
    rows, width = tokens.shape
    top = expert_ids.shape[1]
    part = width // n_dp

    def body(member_ref, tokens_hbm, ids_hbm, logits_hbm, out_ref, own_ref, ids_ref, logits_ref, sems):
        start = pl.multiple_of(member_ref[0] * part, 128)
        copies = [
            pltpu.make_async_copy(tokens_hbm.at[:, pl.ds(start, part)], own_ref, sems.at[0]),
            pltpu.make_async_copy(ids_hbm, ids_ref, sems.at[1]),
            pltpu.make_async_copy(logits_hbm, logits_ref, sems.at[2]),
        ]
        for copy in copies:
            copy.start()
        for copy in copies:
            copy.wait()
        own = own_ref[...]
        scores = 1.0 / (1.0 + jnp.exp(-logits_ref[...]))
        weights = route_scale * scores / jnp.sum(scores, axis=0, keepdims=True)
        high = weights.astype(bf16).astype(f32)
        side = jnp.concatenate(
            [ids_ref[...].astype(f32), high, weights - high, jnp.zeros((SIDE - 3 * top, rows), f32)], axis=0
        )
        side = side.T.astype(bf16)
        for z in range(peers):
            out_ref[z, :, :part] = own
            out_ref[z, :, part:] = side

    outs = [((peers, rows, part + SIDE), bf16)]
    scratch = [
        pltpu.VMEM((rows, part), bf16),
        pltpu.VMEM((top, rows), i32),
        pltpu.VMEM((top, rows), f32),
        pltpu.SemaphoreType.DMA((3,)),
    ]
    return call(body, outs, [SMEM, HBM, HBM, HBM], scratch, None)(member, tokens, expert_ids.T, route_logits.T)


def route_rows(near, far, plane, rows, top, n_x, n_z, n_c, n_dp):
    total = 2 * near.shape[0]
    part = near.shape[1] - SIDE
    experts = n_x * n_c
    held = n_z * SLOTS
    pad = max(16, experts)

    def body(plane_ref, near_ref, far_ref, out_ref, high_ref, low_ref, pick_ref):
        side = jnp.concatenate([near_ref[:, part:], far_ref[:, part:]], axis=0).astype(f32).T
        line = lax.broadcasted_iota(i32, (pad, 1), 0)
        name = ((line // n_c) * n_z + plane_ref[0]) * n_c + line % n_c
        name = jnp.where(line < experts, name, -1).astype(f32)
        named = jnp.zeros((pad, total), f32)
        high = jnp.zeros((pad, total), f32)
        low = jnp.zeros((pad, total), f32)
        for k in range(top):
            same = side[k : k + 1, :] == name
            named = named + jnp.where(same, 1.0, 0.0)
            high = high + jnp.where(same, side[top + k : top + k + 1, :], 0.0)
            low = low + jnp.where(same, side[2 * top + k : 2 * top + k + 1, :], 0.0)
        one = lax.broadcasted_iota(i32, (total, total), 0)
        two = lax.broadcasted_iota(i32, (total, total), 1)
        ahead = jnp.where((one // rows == two // rows) & (one < two), 1.0, 0.0).astype(bf16)
        rank = jnp.dot(named.astype(bf16), ahead, preferred_element_type=f32)
        rank = jnp.where(named > 0.5, rank, -1.0)
        spot = lax.broadcasted_iota(i32, (held, total), 0)
        token = lax.broadcasted_iota(i32, (held, total), 1)
        wanted = jnp.where(token // rows == spot // SLOTS, spot % SLOTS, -2).astype(f32)
        for j in range(experts):
            hit = rank[j : j + 1, :] == wanted
            at = slice(j * held, (j + 1) * held)
            pick_ref[at, :] = jnp.where(hit, 1.0, 0.0).astype(bf16)
            high_ref[at, :] = jnp.where(hit, high[j : j + 1, :], 0.0).astype(bf16)
            low_ref[at, :] = jnp.where(hit, low[j : j + 1, :], 0.0).astype(bf16)
        own = jnp.concatenate([near_ref[:, :part], far_ref[:, :part]], axis=0)
        sent = jnp.dot(pick_ref[...], own, preferred_element_type=f32).astype(bf16)
        for d in range(n_dp):
            out_ref[d] = sent

    slots = experts * held
    outs = (((n_dp, slots, part), bf16),) + (((slots, total), bf16),) * 2
    scratch = [pltpu.VMEM((slots, total), bf16)]
    return call(body, outs, [SMEM, VMEM, VMEM], scratch)(plane, near, far)


def hidden_rows(received, w_gate, w_up):
    n_dp, slots, part = received.shape
    units = w_gate.shape[1]

    def body(rows_ref, gate_ref, up_ref, out_ref):
        v = jnp.zeros((slots, units), f32)
        u = jnp.zeros((slots, units), f32)
        for d in range(n_dp):
            rows = rows_ref[d]
            at = slice(d * part, (d + 1) * part)
            v = v + jnp.dot(rows, gate_ref[at, :], preferred_element_type=f32)
            u = u + jnp.dot(rows, up_ref[at, :], preferred_element_type=f32)
        made = (v / (1.0 + jnp.exp(-v)) * u).astype(bf16)
        for d in range(n_dp):
            out_ref[d] = made

    return call(body, [((n_dp, slots, units), bf16)], [VMEM] * 3)(received, w_gate, w_up)


def output_rows(hidden, downs, member):
    n_dp, slots, _ = hidden.shape
    part = downs[0].shape[1]

    def body(member_ref, hidden_ref, *refs):
        out_ref = refs[-1]
        total = jnp.zeros((slots, part), f32)
        for s in range(n_dp):
            source = lax.rem(member_ref[0] + (n_dp - s), n_dp)
            total = total + jnp.dot(hidden_ref[source], refs[s][...], preferred_element_type=f32)
        out_ref[...] = total.astype(bf16)

    return call(body, [((slots, part), bf16)], [SMEM, VMEM] + [VMEM] * n_dp)(
        member, hidden, *downs
    )


def mix_rows(received, high, low):
    _, part = received.shape
    half = high.shape[1] // 2

    def body(rows_ref, high_ref, low_ref, kept_ref, sent_ref):
        rows = rows_ref[...]
        dims = (((0,), (0,)), ((), ()))
        mixed = lax.dot_general(high_ref[...], rows, dims, preferred_element_type=f32)
        mixed = mixed + lax.dot_general(low_ref[...], rows, dims, preferred_element_type=f32)
        kept_ref[...] = mixed[:half, :]
        sent_ref[...] = mixed[half:, :].astype(bf16)

    return call(body, (((half, part), f32), ((half, part), bf16)), [VMEM] * 3)(received, high, low)


def add_pair(kept, received, share):
    total, part = kept.shape

    def body(kept_ref, received_ref, out_ref):
        both = kept_ref[...] + received_ref[...].astype(f32)
        for i in range(total // share):
            out_ref[i] = both[i * share : (i + 1) * share, :].astype(bf16)

    return call(body, [((total // share, share, part), bf16)], [VMEM] * 2)(kept, received)


def sum_rows(shares, n_dp):
    peers, share, part = shares.shape

    def body(shares_ref, out_ref):
        for d in range(n_dp):
            total = shares_ref[d].astype(f32)
            for z in range(1, peers // n_dp):
                total = total + shares_ref[z * n_dp + d].astype(f32)
            out_ref[:, d * part : (d + 1) * part] = total.astype(bf16)

    return call(body, [((share, n_dp * part), bf16)], [VMEM])(shares)


def exchange(value, axes):
    return lax.all_to_all(value, axes, split_axis=0, concat_axis=0, tiled=True)


def on_device(tokens, expert_ids, route_logits, expert_gate, expert_up, expert_down):
    rows, width = tokens.shape
    top = expert_ids.shape[1]
    n_x, n_pair, n_c, n_dp = (lax.axis_size(a) for a in ("x", "zh", "c", "y"))
    n_z = 2 * n_pair
    part = width // n_dp
    held = n_z * SLOTS
    slots = n_x * n_c * held
    member = lax.axis_index("y").astype(i32)
    member_ref = member.reshape(1)
    plane_ref = (2 * lax.axis_index("zh") + lax.axis_index("zl")).astype(i32).reshape(1)
    w_gate, w_up = expert_gate[0], expert_up[0]

    packed = pack_rows(tokens, expert_ids, route_logits, member_ref, n_dp, n_pair)
    near = exchange(packed, "zh").reshape(n_pair * rows, -1)
    far = lax.ppermute(near, "zl", [(0, 1), (1, 0)])

    downs = []
    for s in range(n_dp):
        owner = member + s
        owner = jnp.where(owner >= n_dp, owner - n_dp, owner)
        piece = lax.dynamic_slice_in_dim(expert_down[0], owner * part, part, axis=1)
        if s:
            piece = lax.ppermute(piece, "y", [(i, (i + s) % n_dp) for i in range(n_dp)])
        downs.append(piece)

    outgoing, high, low = route_rows(
        near, far, plane_ref, rows, top, n_x, n_z, n_c, n_dp
    )
    arrived = exchange(outgoing.reshape(n_dp * n_x * n_c, held, part), ("y", "x", "c"))
    hidden = hidden_rows(arrived.reshape(n_dp, slots, part), w_gate, w_up)
    hidden, downs = lax.optimization_barrier((hidden, downs))
    hidden = exchange(hidden, "y")
    results = output_rows(hidden, downs, member_ref)
    back = exchange(results.reshape(n_x * n_c, held, part), ("x", "c"))
    kept, sent = mix_rows(back.reshape(slots, part), high, low)
    sent = lax.ppermute(sent, "zl", [(0, 1), (1, 0)])
    shares = exchange(add_pair(kept, sent, rows // n_dp), ("zh", "y"))
    return sum_rows(shares, n_dp)


def solution(mesh):
    n_ep, n_dp = mesh.devices.shape
    grid = mesh.devices.reshape(CHIPS_X, n_ep // (CHIPS_X * 2 * CORES), 2, CORES, n_dp)
    fine = Mesh(grid, ("x", "zh", "zl", "c", "y"))
    ep = ("x", "zh", "zl", "c")
    placed = (
        P(ep, None),
        P(ep, None),
        P(ep, None),
        P(ep, None, "y"),
        P(ep, None, "y"),
        P(ep, "y", None),
    )
    return jax.shard_map(
        on_device, mesh=fine, in_specs=placed, out_specs=P(ep + ("y",), None), check_vma=False
    )
```

```python
import jax
import jax.numpy as jnp
from jax import lax
from jax.experimental import pallas as pl
from jax.experimental.pallas import tpu as pltpu
from jax.sharding import Mesh, PartitionSpec as P


route_scale = 2.5
SIDE = 128
SLOTS = 4
CHIPS_X, CORES = 4, 2

f32, bf16, i32 = jnp.float32, jnp.bfloat16, jnp.int32
PARAMS = pltpu.CompilerParams(vmem_limit_bytes=20 * 1024 * 1024)
VMEM = pl.BlockSpec(memory_space=pltpu.VMEM)
HBM = pl.BlockSpec(memory_space=pltpu.HBM)
SMEM = pl.BlockSpec(memory_space=pltpu.SMEM)


def call(body, outs, ins, scratch=(), params=PARAMS):
    many = isinstance(outs, tuple)
    return pl.pallas_call(
        body,
        out_shape=tuple(jax.ShapeDtypeStruct(*o) for o in outs) if many else jax.ShapeDtypeStruct(*outs[0]),
        in_specs=ins,
        out_specs=(VMEM,) * len(outs) if many else VMEM,
        scratch_shapes=list(scratch),
        compiler_params=params,
    )


def pack_rows(tokens, expert_ids, route_logits, member, n_dp, peers):
    rows, width = tokens.shape
    top = expert_ids.shape[1]
    part = width // n_dp

    def body(member_ref, tokens_hbm, ids_hbm, logits_hbm, out_ref, own_ref, ids_ref, logits_ref, sems):
        start = pl.multiple_of(member_ref[0] * part, 128)
        copies = [
            pltpu.make_async_copy(tokens_hbm.at[:, pl.ds(start, part)], own_ref, sems.at[0]),
            pltpu.make_async_copy(ids_hbm, ids_ref, sems.at[1]),
            pltpu.make_async_copy(logits_hbm, logits_ref, sems.at[2]),
        ]
        for copy in copies:
            copy.start()
        for copy in copies:
            copy.wait()
        own = own_ref[...]
        scores = 1.0 / (1.0 + jnp.exp(-logits_ref[...]))
        weights = route_scale * scores / jnp.sum(scores, axis=0, keepdims=True)
        high = weights.astype(bf16).astype(f32)
        side = jnp.concatenate(
            [ids_ref[...].astype(f32), high, weights - high, jnp.zeros((SIDE - 3 * top, rows), f32)], axis=0
        )
        side = side.T.astype(bf16)
        for z in range(peers):
            out_ref[z, :, :part] = own
            out_ref[z, :, part:] = side

    outs = [((peers, rows, part + SIDE), bf16)]
    scratch = [
        pltpu.VMEM((rows, part), bf16),
        pltpu.VMEM((top, rows), i32),
        pltpu.VMEM((top, rows), f32),
        pltpu.SemaphoreType.DMA((3,)),
    ]
    return call(body, outs, [SMEM, HBM, HBM, HBM], scratch, None)(member, tokens, expert_ids.T, route_logits.T)


def route_rows(near, far, plane, rows, top, n_x, n_z, n_c, n_dp):
    total = 2 * near.shape[0]
    part = near.shape[1] - SIDE
    experts = n_x * n_c
    held = n_z * SLOTS
    pad = max(16, experts)

    def body(plane_ref, near_ref, far_ref, out_ref, high_ref, low_ref, pick_ref):
        side = jnp.concatenate([near_ref[:, part:], far_ref[:, part:]], axis=0).astype(f32).T
        line = lax.broadcasted_iota(i32, (pad, 1), 0)
        name = ((line // n_c) * n_z + plane_ref[0]) * n_c + line % n_c
        name = jnp.where(line < experts, name, -1).astype(f32)
        named = jnp.zeros((pad, total), f32)
        high = jnp.zeros((pad, total), f32)
        low = jnp.zeros((pad, total), f32)
        for k in range(top):
            same = side[k : k + 1, :] == name
            named = named + jnp.where(same, 1.0, 0.0)
            high = high + jnp.where(same, side[top + k : top + k + 1, :], 0.0)
            low = low + jnp.where(same, side[2 * top + k : 2 * top + k + 1, :], 0.0)
        one = lax.broadcasted_iota(i32, (total, total), 0)
        two = lax.broadcasted_iota(i32, (total, total), 1)
        ahead = jnp.where((one // rows == two // rows) & (one < two), 1.0, 0.0).astype(bf16)
        rank = jnp.dot(named.astype(bf16), ahead, preferred_element_type=f32)
        rank = jnp.where(named > 0.5, rank, -1.0)
        spot = lax.broadcasted_iota(i32, (held, total), 0)
        token = lax.broadcasted_iota(i32, (held, total), 1)
        wanted = jnp.where(token // rows == spot // SLOTS, spot % SLOTS, -2).astype(f32)
        for j in range(experts):
            hit = rank[j : j + 1, :] == wanted
            at = slice(j * held, (j + 1) * held)
            pick_ref[at, :] = jnp.where(hit, 1.0, 0.0).astype(bf16)
            high_ref[at, :] = jnp.where(hit, high[j : j + 1, :], 0.0).astype(bf16)
            low_ref[at, :] = jnp.where(hit, low[j : j + 1, :], 0.0).astype(bf16)
        own = jnp.concatenate([near_ref[:, :part], far_ref[:, :part]], axis=0)
        sent = jnp.dot(pick_ref[...], own, preferred_element_type=f32).astype(bf16)
        for d in range(n_dp):
            out_ref[d] = sent

    slots = experts * held
    outs = (((n_dp, slots, part), bf16),) + (((slots, total), bf16),) * 2
    scratch = [pltpu.VMEM((slots, total), bf16)]
    return call(body, outs, [SMEM, VMEM, VMEM], scratch)(plane, near, far)


def hidden_rows(received, w_gate, w_up):
    n_dp, slots, part = received.shape
    units = w_gate.shape[1]

    def body(rows_ref, gate_ref, up_ref, out_ref):
        v = jnp.zeros((slots, units), f32)
        u = jnp.zeros((slots, units), f32)
        for d in range(n_dp):
            rows = rows_ref[d]
            at = slice(d * part, (d + 1) * part)
            v = v + jnp.dot(rows, gate_ref[at, :], preferred_element_type=f32)
            u = u + jnp.dot(rows, up_ref[at, :], preferred_element_type=f32)
        made = (v / (1.0 + jnp.exp(-v)) * u).astype(bf16)
        for d in range(n_dp):
            out_ref[d] = made

    return call(body, [((n_dp, slots, units), bf16)], [VMEM] * 3)(received, w_gate, w_up)


def output_rows(hidden, downs, member):
    n_dp, slots, _ = hidden.shape
    part = downs[0].shape[1]

    def body(member_ref, hidden_ref, *refs):
        out_ref = refs[-1]
        total = jnp.zeros((slots, part), f32)
        for s in range(n_dp):
            source = lax.rem(member_ref[0] + (n_dp - s), n_dp)
            total = total + jnp.dot(hidden_ref[source], refs[s][...], preferred_element_type=f32)
        out_ref[...] = total.astype(bf16)

    return call(body, [((slots, part), bf16)], [SMEM, VMEM] + [VMEM] * n_dp)(
        member, hidden, *downs
    )


def cut_columns(down, member, n_dp, shifts):
    units, width = down.shape
    part = width // n_dp

    def body(member_ref, down_hbm, *refs):
        sems = refs[-1]
        copies = []
        for i, s in enumerate(shifts):
            owner = lax.rem(member_ref[0] + s, n_dp)
            start = pl.multiple_of(owner * part, 128)
            copies.append(pltpu.make_async_copy(down_hbm.at[:, pl.ds(start, part)], refs[i], sems.at[i]))
        for copy in copies:
            copy.start()
        for copy in copies:
            copy.wait()

    count = len(shifts)
    return pl.pallas_call(
        body,
        out_shape=(jax.ShapeDtypeStruct((units, part), bf16),) * count,
        in_specs=[SMEM, HBM],
        out_specs=(HBM,) * count,
        scratch_shapes=[pltpu.SemaphoreType.DMA((count,))],
        name="cut_columns",
    )(member, down)


def mix_rows(received, high, low):
    _, part = received.shape
    half = high.shape[1] // 2

    def body(rows_ref, high_ref, low_ref, kept_ref, sent_ref):
        rows = rows_ref[...]
        dims = (((0,), (0,)), ((), ()))
        mixed = lax.dot_general(high_ref[...], rows, dims, preferred_element_type=f32)
        mixed = mixed + lax.dot_general(low_ref[...], rows, dims, preferred_element_type=f32)
        kept_ref[...] = mixed[:half, :]
        sent_ref[...] = mixed[half:, :].astype(bf16)

    return call(body, (((half, part), f32), ((half, part), bf16)), [VMEM] * 3)(received, high, low)


def add_pair(kept, received, share):
    total, part = kept.shape

    def body(kept_ref, received_ref, out_ref):
        both = kept_ref[...] + received_ref[...].astype(f32)
        for i in range(total // share):
            out_ref[i] = both[i * share : (i + 1) * share, :].astype(bf16)

    return call(body, [((total // share, share, part), bf16)], [VMEM] * 2)(kept, received)


def sum_rows(shares, n_dp):
    peers, share, part = shares.shape

    def body(shares_ref, out_ref):
        for d in range(n_dp):
            total = shares_ref[d].astype(f32)
            for z in range(1, peers // n_dp):
                total = total + shares_ref[z * n_dp + d].astype(f32)
            out_ref[:, d * part : (d + 1) * part] = total.astype(bf16)

    return call(body, [((share, n_dp * part), bf16)], [VMEM])(shares)


def exchange(value, axes):
    return lax.all_to_all(value, axes, split_axis=0, concat_axis=0, tiled=True)


def on_device(tokens, expert_ids, route_logits, expert_gate, expert_up, expert_down):
    rows, width = tokens.shape
    top = expert_ids.shape[1]
    n_x, n_pair, n_c, n_dp = (lax.axis_size(a) for a in ("x", "zh", "c", "y"))
    n_z = 2 * n_pair
    part = width // n_dp
    held = n_z * SLOTS
    slots = n_x * n_c * held
    member = lax.axis_index("y").astype(i32)
    member_ref = member.reshape(1)
    plane_ref = (2 * lax.axis_index("zh") + lax.axis_index("zl")).astype(i32).reshape(1)
    w_gate, w_up = expert_gate[0], expert_up[0]

    packed = pack_rows(tokens, expert_ids, route_logits, member_ref, n_dp, n_pair)
    near = exchange(packed, "zh").reshape(n_pair * rows, -1)
    far = lax.ppermute(near, "zl", [(0, 1), (1, 0)])

    early = cut_columns(expert_down[0], member_ref, n_dp, range(1, n_dp - 1))
    late = cut_columns(expert_down[0], member_ref, n_dp, (0, n_dp - 1))
    downs = [late[0], *early, late[1]]
    for s in range(1, n_dp):
        downs[s] = lax.ppermute(downs[s], "y", [(i, (i + s) % n_dp) for i in range(n_dp)])

    outgoing, high, low = route_rows(
        near, far, plane_ref, rows, top, n_x, n_z, n_c, n_dp
    )
    arrived = exchange(outgoing.reshape(n_dp * n_x * n_c, held, part), ("y", "x", "c"))
    hidden = hidden_rows(arrived.reshape(n_dp, slots, part), w_gate, w_up)
    hidden, downs = lax.optimization_barrier((hidden, downs))
    hidden = exchange(hidden, "y")
    results = output_rows(hidden, downs, member_ref)
    back = exchange(results.reshape(n_x * n_c, held, part), ("x", "c"))
    kept, sent = mix_rows(back.reshape(slots, part), high, low)
    sent = lax.ppermute(sent, "zl", [(0, 1), (1, 0)])
    shares = exchange(add_pair(kept, sent, rows // n_dp), ("zh", "y"))
    return sum_rows(shares, n_dp)


def solution(mesh):
    n_ep, n_dp = mesh.devices.shape
    grid = mesh.devices.reshape(CHIPS_X, n_ep // (CHIPS_X * 2 * CORES), 2, CORES, n_dp)
    fine = Mesh(grid, ("x", "zh", "zl", "c", "y"))
    ep = ("x", "zh", "zl", "c")
    placed = (
        P(ep, None),
        P(ep, None),
        P(ep, None),
        P(ep, None, "y"),
        P(ep, None, "y"),
        P(ep, "y", None),
    )
    return jax.shard_map(
        on_device, mesh=fine, in_specs=placed, out_specs=P(ep + ("y",), None), check_vma=False
    )
```

```python
import jax
import jax.numpy as jnp
from jax import lax
from jax.experimental import pallas as pl
from jax.experimental.pallas import tpu as pltpu
from jax.sharding import Mesh, PartitionSpec as P


route_scale = 2.5
SIDE = 128
SLOTS = 4
CHIPS_X, CORES = 4, 2

f32, bf16, i32 = jnp.float32, jnp.bfloat16, jnp.int32
PARAMS = pltpu.CompilerParams(vmem_limit_bytes=20 * 1024 * 1024)
VMEM = pl.BlockSpec(memory_space=pltpu.VMEM)
HBM = pl.BlockSpec(memory_space=pltpu.HBM)
SMEM = pl.BlockSpec(memory_space=pltpu.SMEM)


def call(body, outs, ins, scratch=(), params=PARAMS):
    many = isinstance(outs, tuple)
    return pl.pallas_call(
        body,
        out_shape=tuple(jax.ShapeDtypeStruct(*o) for o in outs) if many else jax.ShapeDtypeStruct(*outs[0]),
        in_specs=ins,
        out_specs=(VMEM,) * len(outs) if many else VMEM,
        scratch_shapes=list(scratch),
        compiler_params=params,
    )


def pack_rows(tokens, expert_ids, route_logits, member, n_dp, peers):
    rows, width = tokens.shape
    top = expert_ids.shape[1]
    part = width // n_dp

    def body(member_ref, tokens_hbm, ids_hbm, logits_hbm, out_ref, own_ref, ids_ref, logits_ref, sems):
        start = pl.multiple_of(member_ref[0] * part, 128)
        copies = [
            pltpu.make_async_copy(tokens_hbm.at[:, pl.ds(start, part)], own_ref, sems.at[0]),
            pltpu.make_async_copy(ids_hbm, ids_ref, sems.at[1]),
            pltpu.make_async_copy(logits_hbm, logits_ref, sems.at[2]),
        ]
        for copy in copies:
            copy.start()
        for copy in copies:
            copy.wait()
        own = own_ref[...]
        scores = 1.0 / (1.0 + jnp.exp(-logits_ref[...]))
        weights = route_scale * scores / jnp.sum(scores, axis=0, keepdims=True)
        high = weights.astype(bf16).astype(f32)
        side = jnp.concatenate(
            [ids_ref[...].astype(f32), high, weights - high, jnp.zeros((SIDE - 3 * top, rows), f32)], axis=0
        )
        side = side.T.astype(bf16)
        for z in range(peers):
            out_ref[z, :, :part] = own
            out_ref[z, :, part:] = side

    outs = [((peers, rows, part + SIDE), bf16)]
    scratch = [
        pltpu.VMEM((rows, part), bf16),
        pltpu.VMEM((top, rows), i32),
        pltpu.VMEM((top, rows), f32),
        pltpu.SemaphoreType.DMA((3,)),
    ]
    return call(body, outs, [SMEM, HBM, HBM, HBM], scratch, None)(member, tokens, expert_ids.T, route_logits.T)


def route_rows(near, far, plane, rows, top, n_x, n_z, n_c, n_dp):
    total = 2 * near.shape[0]
    part = near.shape[1] - SIDE
    experts = n_x * n_c
    held = n_z * SLOTS
    pad = max(16, experts)

    def body(plane_ref, near_ref, far_ref, out_ref, high_ref, low_ref, pick_ref):
        side = jnp.concatenate([near_ref[:, part:], far_ref[:, part:]], axis=0).astype(f32).T
        line = lax.broadcasted_iota(i32, (pad, 1), 0)
        name = ((line // n_c) * n_z + plane_ref[0]) * n_c + line % n_c
        name = jnp.where(line < experts, name, -1).astype(f32)
        named = jnp.zeros((pad, total), f32)
        high = jnp.zeros((pad, total), f32)
        low = jnp.zeros((pad, total), f32)
        for k in range(top):
            same = side[k : k + 1, :] == name
            named = named + jnp.where(same, 1.0, 0.0)
            high = high + jnp.where(same, side[top + k : top + k + 1, :], 0.0)
            low = low + jnp.where(same, side[2 * top + k : 2 * top + k + 1, :], 0.0)
        one = lax.broadcasted_iota(i32, (total, total), 0)
        two = lax.broadcasted_iota(i32, (total, total), 1)
        ahead = jnp.where((one // rows == two // rows) & (one < two), 1.0, 0.0).astype(bf16)
        rank = jnp.dot(named.astype(bf16), ahead, preferred_element_type=f32)
        rank = jnp.where(named > 0.5, rank, -1.0)
        spot = lax.broadcasted_iota(i32, (held, total), 0)
        token = lax.broadcasted_iota(i32, (held, total), 1)
        wanted = jnp.where(token // rows == spot // SLOTS, spot % SLOTS, -2).astype(f32)
        for j in range(experts):
            hit = rank[j : j + 1, :] == wanted
            at = slice(j * held, (j + 1) * held)
            pick_ref[at, :] = jnp.where(hit, 1.0, 0.0).astype(bf16)
            high_ref[at, :] = jnp.where(hit, high[j : j + 1, :], 0.0).astype(bf16)
            low_ref[at, :] = jnp.where(hit, low[j : j + 1, :], 0.0).astype(bf16)
        own = jnp.concatenate([near_ref[:, :part], far_ref[:, :part]], axis=0)
        sent = jnp.dot(pick_ref[...], own, preferred_element_type=f32).astype(bf16)
        for d in range(n_dp):
            out_ref[d] = sent

    slots = experts * held
    outs = (((n_dp, slots, part), bf16),) + (((slots, total), bf16),) * 2
    scratch = [pltpu.VMEM((slots, total), bf16)]
    return call(body, outs, [SMEM, VMEM, VMEM], scratch)(plane, near, far)


def hidden_rows(received, w_gate, w_up):
    n_dp, slots, part = received.shape
    units = w_gate.shape[1]

    def body(rows_ref, gate_ref, up_ref, out_ref):
        v = jnp.zeros((slots, units), f32)
        u = jnp.zeros((slots, units), f32)
        for d in range(n_dp):
            rows = rows_ref[d]
            at = slice(d * part, (d + 1) * part)
            v = v + jnp.dot(rows, gate_ref[at, :], preferred_element_type=f32)
            u = u + jnp.dot(rows, up_ref[at, :], preferred_element_type=f32)
        made = (v / (1.0 + jnp.exp(-v)) * u).astype(bf16)
        for d in range(n_dp):
            out_ref[d] = made

    return call(body, [((n_dp, slots, units), bf16)], [VMEM] * 3)(received, w_gate, w_up)


def output_rows(hidden, downs, member):
    n_dp, slots, _ = hidden.shape
    part = downs[0].shape[1]

    def body(member_ref, hidden_ref, *refs):
        out_ref = refs[-1]
        total = jnp.zeros((slots, part), f32)
        for s in range(n_dp):
            source = lax.rem(member_ref[0] + (n_dp - s), n_dp)
            total = total + jnp.dot(hidden_ref[source], refs[s][...], preferred_element_type=f32)
        out_ref[...] = total.astype(bf16)

    return call(body, [((slots, part), bf16)], [SMEM, VMEM] + [VMEM] * n_dp)(
        member, hidden, *downs
    )


def cut_columns(down, member, n_dp, shifts):
    units, width = down.shape
    part = width // n_dp

    def body(member_ref, down_hbm, *refs):
        sems = refs[-1]
        copies = []
        for i, s in enumerate(shifts):
            owner = lax.rem(member_ref[0] + s, n_dp)
            start = pl.multiple_of(owner * part, 128)
            copies.append(pltpu.make_async_copy(down_hbm.at[:, pl.ds(start, part)], refs[i], sems.at[i]))
        for copy in copies:
            copy.start()
        for copy in copies:
            copy.wait()

    count = len(shifts)
    outs = (((units, part), bf16),) * count
    return call(body, outs, [SMEM, HBM], [pltpu.SemaphoreType.DMA((count,))], None)(member, down)


def mix_rows(received, high, low):
    _, part = received.shape
    half = high.shape[1] // 2

    def body(rows_ref, high_ref, low_ref, kept_ref, sent_ref):
        rows = rows_ref[...]
        dims = (((0,), (0,)), ((), ()))
        mixed = lax.dot_general(high_ref[...], rows, dims, preferred_element_type=f32)
        mixed = mixed + lax.dot_general(low_ref[...], rows, dims, preferred_element_type=f32)
        kept_ref[...] = mixed[:half, :]
        sent_ref[...] = mixed[half:, :].astype(bf16)

    return call(body, (((half, part), f32), ((half, part), bf16)), [VMEM] * 3)(received, high, low)


def add_pair(kept, received, share):
    total, part = kept.shape

    def body(kept_ref, received_ref, out_ref):
        both = kept_ref[...] + received_ref[...].astype(f32)
        for i in range(total // share):
            out_ref[i] = both[i * share : (i + 1) * share, :].astype(bf16)

    return call(body, [((total // share, share, part), bf16)], [VMEM] * 2)(kept, received)


def sum_rows(shares, n_dp):
    peers, share, part = shares.shape

    def body(shares_ref, out_ref):
        for d in range(n_dp):
            total = shares_ref[d].astype(f32)
            for z in range(1, peers // n_dp):
                total = total + shares_ref[z * n_dp + d].astype(f32)
            out_ref[:, d * part : (d + 1) * part] = total.astype(bf16)

    return call(body, [((share, n_dp * part), bf16)], [VMEM])(shares)


def exchange(value, axes):
    return lax.all_to_all(value, axes, split_axis=0, concat_axis=0, tiled=True)


def on_device(tokens, expert_ids, route_logits, expert_gate, expert_up, expert_down):
    rows, width = tokens.shape
    top = expert_ids.shape[1]
    n_x, n_pair, n_c, n_dp = (lax.axis_size(a) for a in ("x", "zh", "c", "y"))
    n_z = 2 * n_pair
    part = width // n_dp
    held = n_z * SLOTS
    slots = n_x * n_c * held
    member = lax.axis_index("y").astype(i32)
    member_ref = member.reshape(1)
    plane_ref = (2 * lax.axis_index("zh") + lax.axis_index("zl")).astype(i32).reshape(1)
    w_gate, w_up = expert_gate[0], expert_up[0]

    packed = pack_rows(tokens, expert_ids, route_logits, member_ref, n_dp, n_pair)
    near = exchange(packed, "zh").reshape(n_pair * rows, -1)
    far = lax.ppermute(near, "zl", [(0, 1), (1, 0)])

    early = cut_columns(expert_down[0], member_ref, n_dp, range(1, n_dp - 1))
    late = cut_columns(expert_down[0], member_ref, n_dp, (0, n_dp - 1))
    downs = [late[0], *early, late[1]]
    for s in range(1, n_dp):
        downs[s] = lax.ppermute(downs[s], "y", [(i, (i + s) % n_dp) for i in range(n_dp)])

    outgoing, high, low = route_rows(
        near, far, plane_ref, rows, top, n_x, n_z, n_c, n_dp
    )
    arrived = exchange(outgoing.reshape(n_dp * n_x * n_c, held, part), ("y", "x", "c"))
    hidden = hidden_rows(arrived.reshape(n_dp, slots, part), w_gate, w_up)
    hidden, downs = lax.optimization_barrier((hidden, downs))
    hidden = exchange(hidden, "y")
    results = output_rows(hidden, downs, member_ref)
    back = exchange(results.reshape(n_x * n_c, held, part), ("x", "c"))
    kept, sent = mix_rows(back.reshape(slots, part), high, low)
    sent = lax.ppermute(sent, "zl", [(0, 1), (1, 0)])
    shares = exchange(add_pair(kept, sent, rows // n_dp), ("zh", "y"))
    return sum_rows(shares, n_dp)


def solution(mesh):
    n_ep, n_dp = mesh.devices.shape
    grid = mesh.devices.reshape(CHIPS_X, n_ep // (CHIPS_X * 2 * CORES), 2, CORES, n_dp)
    fine = Mesh(grid, ("x", "zh", "zl", "c", "y"))
    ep = ("x", "zh", "zl", "c")
    placed = (
        P(ep, None),
        P(ep, None),
        P(ep, None),
        P(ep, None, "y"),
        P(ep, None, "y"),
        P(ep, "y", None),
    )
    return jax.shard_map(
        on_device, mesh=fine, in_specs=placed, out_specs=P(ep + ("y",), None), check_vma=False
    )
```

```python
import jax
import jax.numpy as jnp
from jax import lax
from jax.experimental import pallas as pl
from jax.experimental.pallas import tpu as pltpu
from jax.sharding import Mesh, PartitionSpec as P


route_scale = 2.5
SIDE = 128
SLOTS = 4
CHIPS_X, CORES = 4, 2

f32, bf16, i32 = jnp.float32, jnp.bfloat16, jnp.int32
PARAMS = pltpu.CompilerParams(vmem_limit_bytes=20 * 1024 * 1024)
VMEM = pl.BlockSpec(memory_space=pltpu.VMEM)
HBM = pl.BlockSpec(memory_space=pltpu.HBM)
SMEM = pl.BlockSpec(memory_space=pltpu.SMEM)


def call(body, outs, ins, scratch=(), params=PARAMS):
    many = isinstance(outs, tuple)
    return pl.pallas_call(
        body,
        out_shape=tuple(jax.ShapeDtypeStruct(*o) for o in outs) if many else jax.ShapeDtypeStruct(*outs[0]),
        in_specs=ins,
        out_specs=(VMEM,) * len(outs) if many else VMEM,
        scratch_shapes=list(scratch),
        compiler_params=params,
    )


def pack_rows(tokens, expert_ids, route_logits, member, n_dp, peers):
    rows, width = tokens.shape
    top = expert_ids.shape[1]
    part = width // n_dp

    def body(member_ref, tokens_hbm, ids_hbm, logits_hbm, out_ref, own_ref, ids_ref, logits_ref, sems):
        start = pl.multiple_of(member_ref[0] * part, 128)
        copies = [
            pltpu.make_async_copy(tokens_hbm.at[:, pl.ds(start, part)], own_ref, sems.at[0]),
            pltpu.make_async_copy(ids_hbm, ids_ref, sems.at[1]),
            pltpu.make_async_copy(logits_hbm, logits_ref, sems.at[2]),
        ]
        for copy in copies:
            copy.start()
        for copy in copies:
            copy.wait()
        own = own_ref[...]
        scores = 1.0 / (1.0 + jnp.exp(-logits_ref[...]))
        weights = route_scale * scores / jnp.sum(scores, axis=0, keepdims=True)
        high = weights.astype(bf16).astype(f32)
        side = jnp.concatenate(
            [ids_ref[...].astype(f32), high, weights - high, jnp.zeros((SIDE - 3 * top, rows), f32)], axis=0
        )
        side = side.T.astype(bf16)
        for z in range(peers):
            out_ref[z, :, :part] = own
            out_ref[z, :, part:] = side

    outs = [((peers, rows, part + SIDE), bf16)]
    scratch = [
        pltpu.VMEM((rows, part), bf16),
        pltpu.VMEM((top, rows), i32),
        pltpu.VMEM((top, rows), f32),
        pltpu.SemaphoreType.DMA((3,)),
    ]
    return call(body, outs, [SMEM, HBM, HBM, HBM], scratch, None)(member, tokens, expert_ids.T, route_logits.T)


def route_rows(gathered, pair, rows, top, n_x, n_pair, n_c, n_dp):
    total = gathered.shape[0]
    part = gathered.shape[1] - SIDE
    experts = n_x * 2 * n_c
    held = n_pair * SLOTS
    pad = max(16, experts)

    def body(pair_ref, gathered_ref, out_ref, high_ref, low_ref, pick_ref):
        side = gathered_ref[:, part:].astype(f32).T
        line = lax.broadcasted_iota(i32, (pad, 1), 0)
        name = ((line // (2 * n_c)) * n_pair + pair_ref[0]) * (2 * n_c) + line % (2 * n_c)
        name = jnp.where(line < experts, name, -1).astype(f32)
        named = jnp.zeros((pad, total), f32)
        high = jnp.zeros((pad, total), f32)
        low = jnp.zeros((pad, total), f32)
        for k in range(top):
            same = side[k : k + 1, :] == name
            named = named + jnp.where(same, 1.0, 0.0)
            high = high + jnp.where(same, side[top + k : top + k + 1, :], 0.0)
            low = low + jnp.where(same, side[2 * top + k : 2 * top + k + 1, :], 0.0)
        one = lax.broadcasted_iota(i32, (total, total), 0)
        two = lax.broadcasted_iota(i32, (total, total), 1)
        ahead = jnp.where((one // rows == two // rows) & (one < two), 1.0, 0.0).astype(bf16)
        rank = jnp.dot(named.astype(bf16), ahead, preferred_element_type=f32)
        rank = jnp.where(named > 0.5, rank, -1.0)
        spot = lax.broadcasted_iota(i32, (held, total), 0)
        token = lax.broadcasted_iota(i32, (held, total), 1)
        wanted = jnp.where(token // rows == spot // SLOTS, spot % SLOTS, -2).astype(f32)
        for j in range(experts):
            hit = rank[j : j + 1, :] == wanted
            at = slice(j * held, (j + 1) * held)
            pick_ref[at, :] = jnp.where(hit, 1.0, 0.0).astype(bf16)
            high_ref[at, :] = jnp.where(hit, high[j : j + 1, :], 0.0).astype(bf16)
            low_ref[at, :] = jnp.where(hit, low[j : j + 1, :], 0.0).astype(bf16)
        sent = jnp.dot(pick_ref[...], gathered_ref[:, :part], preferred_element_type=f32).astype(bf16)
        for d in range(n_dp):
            out_ref[d] = sent

    slots = experts * held
    outs = (((n_dp, slots, part), bf16),) + (((slots, total), bf16),) * 2
    scratch = [pltpu.VMEM((slots, total), bf16)]
    return call(body, outs, [SMEM, VMEM], scratch)(pair, gathered)


def hidden_rows(received, w_gate, w_up):
    n_dp, slots, part = received.shape
    units = w_gate.shape[1]

    def body(rows_ref, gate_ref, up_ref, out_ref):
        v = jnp.zeros((slots, units), f32)
        u = jnp.zeros((slots, units), f32)
        for d in range(n_dp):
            rows = rows_ref[d]
            at = slice(d * part, (d + 1) * part)
            v = v + jnp.dot(rows, gate_ref[at, :], preferred_element_type=f32)
            u = u + jnp.dot(rows, up_ref[at, :], preferred_element_type=f32)
        made = (v / (1.0 + jnp.exp(-v)) * u).astype(bf16)
        for d in range(n_dp):
            out_ref[d] = made

    return call(body, [((n_dp, slots, units), bf16)], [VMEM] * 3)(received, w_gate, w_up)


def output_rows(hidden, downs, member):
    n_dp, slots, _ = hidden.shape
    part = downs[0].shape[1]

    def body(member_ref, hidden_ref, *refs):
        out_ref = refs[-1]
        total = jnp.zeros((slots, part), f32)
        for s in range(n_dp):
            source = lax.rem(member_ref[0] + (n_dp - s), n_dp)
            total = total + jnp.dot(hidden_ref[source], refs[s][...], preferred_element_type=f32)
        out_ref[...] = total.astype(bf16)

    return call(body, [((slots, part), bf16)], [SMEM, VMEM] + [VMEM] * n_dp)(
        member, hidden, *downs
    )


def cut_columns(down, member, n_dp, shifts):
    units, width = down.shape
    part = width // n_dp

    def body(member_ref, down_hbm, *refs):
        sems = refs[-1]
        copies = []
        for i, s in enumerate(shifts):
            owner = lax.rem(member_ref[0] + s, n_dp)
            start = pl.multiple_of(owner * part, 128)
            copies.append(pltpu.make_async_copy(down_hbm.at[:, pl.ds(start, part)], refs[i], sems.at[i]))
        for copy in copies:
            copy.start()
        for copy in copies:
            copy.wait()

    count = len(shifts)
    outs = (((units, part), bf16),) * count
    return call(body, outs, [SMEM, HBM], [pltpu.SemaphoreType.DMA((count,))], None)(member, down)


def mix_rows(received, high, low, share):
    _, part = received.shape
    total = high.shape[1]

    def body(rows_ref, high_ref, low_ref, out_ref):
        rows = rows_ref[...]
        dims = (((0,), (0,)), ((), ()))
        mixed = lax.dot_general(high_ref[...], rows, dims, preferred_element_type=f32)
        mixed = mixed + lax.dot_general(low_ref[...], rows, dims, preferred_element_type=f32)
        for i in range(total // share):
            out_ref[i] = mixed[i * share : (i + 1) * share, :].astype(bf16)

    return call(body, [((total // share, share, part), bf16)], [VMEM] * 3)(received, high, low)


def sum_rows(shares, n_dp):
    peers, share, part = shares.shape

    def body(shares_ref, out_ref):
        for d in range(n_dp):
            total = shares_ref[d].astype(f32)
            for z in range(1, peers // n_dp):
                total = total + shares_ref[z * n_dp + d].astype(f32)
            out_ref[:, d * part : (d + 1) * part] = total.astype(bf16)

    return call(body, [((share, n_dp * part), bf16)], [VMEM])(shares)


def exchange(value, axes):
    return lax.all_to_all(value, axes, split_axis=0, concat_axis=0, tiled=True)


def on_device(tokens, expert_ids, route_logits, expert_gate, expert_up, expert_down):
    rows, width = tokens.shape
    top = expert_ids.shape[1]
    n_x, n_pair, n_c, n_dp = (lax.axis_size(a) for a in ("x", "zh", "c", "y"))
    part = width // n_dp
    experts = n_x * 2 * n_c
    held = n_pair * SLOTS
    slots = experts * held
    member = lax.axis_index("y").astype(i32)
    member_ref = member.reshape(1)
    pair_ref = lax.axis_index("zh").astype(i32).reshape(1)
    w_gate, w_up = expert_gate[0], expert_up[0]

    packed = pack_rows(tokens, expert_ids, route_logits, member_ref, n_dp, n_pair)
    gathered = exchange(packed, "zh").reshape(n_pair * rows, -1)

    early = cut_columns(expert_down[0], member_ref, n_dp, range(1, n_dp - 1))
    late = cut_columns(expert_down[0], member_ref, n_dp, (0, n_dp - 1))
    downs = [late[0], *early, late[1]]
    for s in range(1, n_dp):
        downs[s] = lax.ppermute(downs[s], "y", [(i, (i + s) % n_dp) for i in range(n_dp)])

    outgoing, high, low = route_rows(gathered, pair_ref, rows, top, n_x, n_pair, n_c, n_dp)
    arrived = exchange(outgoing.reshape(n_dp * experts, held, part), ("y", "x", "zl", "c"))
    hidden = hidden_rows(arrived.reshape(n_dp, slots, part), w_gate, w_up)
    hidden, downs = lax.optimization_barrier((hidden, downs))
    hidden = exchange(hidden, "y")
    results = output_rows(hidden, downs, member_ref)
    back = exchange(results.reshape(experts, held, part), ("x", "zl", "c"))
    mixed = mix_rows(back.reshape(slots, part), high, low, rows // n_dp)
    shares = exchange(mixed, ("zh", "y"))
    return sum_rows(shares, n_dp)


def solution(mesh):
    n_ep, n_dp = mesh.devices.shape
    grid = mesh.devices.reshape(CHIPS_X, n_ep // (CHIPS_X * 2 * CORES), 2, CORES, n_dp)
    fine = Mesh(grid, ("x", "zh", "zl", "c", "y"))
    ep = ("x", "zh", "zl", "c")
    placed = (
        P(ep, None),
        P(ep, None),
        P(ep, None),
        P(ep, None, "y"),
        P(ep, None, "y"),
        P(ep, "y", None),
    )
    return jax.shard_map(
        on_device, mesh=fine, in_specs=placed, out_specs=P(ep + ("y",), None), check_vma=False
    )
```

```python
import jax
import jax.numpy as jnp
from jax import lax
from jax.experimental import pallas as pl
from jax.experimental.pallas import tpu as pltpu
from jax.sharding import Mesh, PartitionSpec as P


route_scale = 2.5
SIDE = 128
SLOTS = 4
CHIPS_X, CORES = 4, 2

f32, bf16, i32 = jnp.float32, jnp.bfloat16, jnp.int32
PARAMS = pltpu.CompilerParams(vmem_limit_bytes=20 * 1024 * 1024)
VMEM = pl.BlockSpec(memory_space=pltpu.VMEM)
HBM = pl.BlockSpec(memory_space=pltpu.HBM)
SMEM = pl.BlockSpec(memory_space=pltpu.SMEM)


def call(body, outs, ins, scratch=(), params=PARAMS):
    many = isinstance(outs, tuple)
    return pl.pallas_call(
        body,
        out_shape=tuple(jax.ShapeDtypeStruct(*o) for o in outs) if many else jax.ShapeDtypeStruct(*outs[0]),
        in_specs=ins,
        out_specs=(VMEM,) * len(outs) if many else VMEM,
        scratch_shapes=list(scratch),
        compiler_params=params,
    )


def pack_rows(tokens, expert_ids, route_logits, member, n_dp, peers):
    rows, width = tokens.shape
    top = expert_ids.shape[1]
    part = width // n_dp

    def body(member_ref, tokens_hbm, ids_hbm, logits_hbm, out_ref, own_ref, ids_ref, logits_ref, sems):
        start = pl.multiple_of(member_ref[0] * part, 128)
        copies = [
            pltpu.make_async_copy(tokens_hbm.at[:, pl.ds(start, part)], own_ref, sems.at[0]),
            pltpu.make_async_copy(ids_hbm, ids_ref, sems.at[1]),
            pltpu.make_async_copy(logits_hbm, logits_ref, sems.at[2]),
        ]
        for copy in copies:
            copy.start()
        for copy in copies:
            copy.wait()
        own = own_ref[...]
        scores = 1.0 / (1.0 + jnp.exp(-logits_ref[...]))
        weights = route_scale * scores / jnp.sum(scores, axis=0, keepdims=True)
        high = weights.astype(bf16).astype(f32)
        side = jnp.concatenate(
            [ids_ref[...].astype(f32), high, weights - high, jnp.zeros((SIDE - 3 * top, rows), f32)], axis=0
        )
        side = side.T.astype(bf16)
        for z in range(peers):
            out_ref[z, :, :part] = own
            out_ref[z, :, part:] = side

    outs = [((peers, rows, part + SIDE), bf16)]
    scratch = [
        pltpu.VMEM((rows, part), bf16),
        pltpu.VMEM((top, rows), i32),
        pltpu.VMEM((top, rows), f32),
        pltpu.SemaphoreType.DMA((3,)),
    ]
    return call(body, outs, [SMEM, HBM, HBM, HBM], scratch, None)(member, tokens, expert_ids.T, route_logits.T)


def route_masks(pair, total, rows, held):
    def body(pair_ref, ahead_ref, wanted_ref):
        one = lax.broadcasted_iota(i32, (total, total), 0)
        two = lax.broadcasted_iota(i32, (total, total), 1)
        ahead_ref[...] = jnp.where((one // rows == two // rows) & (one < two), 1.0, 0.0).astype(bf16)
        spot = lax.broadcasted_iota(i32, (held, total), 0)
        token = lax.broadcasted_iota(i32, (held, total), 1)
        wanted_ref[...] = jnp.where(token // rows == spot // SLOTS, spot % SLOTS, -2).astype(f32)

    outs = (((total, total), bf16), ((held, total), f32))
    return call(body, outs, [SMEM])(pair)


def route_rows(gathered, pair, ahead, wanted, top, n_x, n_pair, n_c, n_dp):
    total = gathered.shape[0]
    part = gathered.shape[1] - SIDE
    experts = n_x * 2 * n_c
    held = n_pair * SLOTS
    pad = max(16, experts)

    def body(pair_ref, gathered_ref, ahead_ref, wanted_ref, out_ref, high_ref, low_ref, pick_ref):
        side = gathered_ref[:, part:].astype(f32).T
        line = lax.broadcasted_iota(i32, (pad, 1), 0)
        core, chip, side_plane = line // (2 * n_x), line // 2 % n_x, line % 2
        name = ((chip * n_pair + pair_ref[0]) * 2 + side_plane) * n_c + core
        name = jnp.where(line < experts, name, -1).astype(f32)
        named = jnp.zeros((pad, total), f32)
        high = jnp.zeros((pad, total), f32)
        low = jnp.zeros((pad, total), f32)
        for k in range(top):
            same = side[k : k + 1, :] == name
            named = named + jnp.where(same, 1.0, 0.0)
            high = high + jnp.where(same, side[top + k : top + k + 1, :], 0.0)
            low = low + jnp.where(same, side[2 * top + k : 2 * top + k + 1, :], 0.0)
        rank = jnp.dot(named.astype(bf16), ahead_ref[...], preferred_element_type=f32)
        rank = jnp.where(named > 0.5, rank, -1.0)
        wanted = wanted_ref[...]
        for j in range(experts):
            hit = rank[j : j + 1, :] == wanted
            at = slice(j * held, (j + 1) * held)
            pick_ref[at, :] = jnp.where(hit, 1.0, 0.0).astype(bf16)
            high_ref[at, :] = jnp.where(hit, high[j : j + 1, :], 0.0).astype(bf16)
            low_ref[at, :] = jnp.where(hit, low[j : j + 1, :], 0.0).astype(bf16)
        sent = jnp.dot(pick_ref[...], gathered_ref[:, :part], preferred_element_type=f32).astype(bf16)
        for d in range(n_dp):
            out_ref[d] = sent

    slots = experts * held
    outs = (((n_dp, slots, part), bf16),) + (((slots, total), bf16),) * 2
    scratch = [pltpu.VMEM((slots, total), bf16)]
    return call(body, outs, [SMEM] + [VMEM] * 3, scratch)(pair, gathered, ahead, wanted)


def hidden_rows(received, w_gate, w_up):
    n_dp, slots, part = received.shape
    units = w_gate.shape[1]

    def body(rows_ref, gate_ref, up_ref, out_ref):
        v = jnp.zeros((slots, units), f32)
        u = jnp.zeros((slots, units), f32)
        for d in range(n_dp):
            rows = rows_ref[d]
            at = slice(d * part, (d + 1) * part)
            v = v + jnp.dot(rows, gate_ref[at, :], preferred_element_type=f32)
            u = u + jnp.dot(rows, up_ref[at, :], preferred_element_type=f32)
        made = (v / (1.0 + jnp.exp(-v)) * u).astype(bf16)
        for d in range(n_dp):
            out_ref[d] = made

    return call(body, [((n_dp, slots, units), bf16)], [VMEM] * 3)(received, w_gate, w_up)


def output_rows(hidden, downs, member):
    n_dp, slots, _ = hidden.shape
    part = downs[0].shape[1]

    def body(member_ref, hidden_ref, *refs):
        out_ref = refs[-1]
        total = jnp.zeros((slots, part), f32)
        for s in range(n_dp):
            source = lax.rem(member_ref[0] + (n_dp - s), n_dp)
            total = total + jnp.dot(hidden_ref[source], refs[s][...], preferred_element_type=f32)
        out_ref[...] = total.astype(bf16)

    return call(body, [((slots, part), bf16)], [SMEM, VMEM] + [VMEM] * n_dp)(
        member, hidden, *downs
    )


def mix_rows(received, high, low, share):
    _, part = received.shape
    total = high.shape[1]

    def body(rows_ref, high_ref, low_ref, out_ref):
        rows = rows_ref[...]
        dims = (((0,), (0,)), ((), ()))
        mixed = lax.dot_general(high_ref[...], rows, dims, preferred_element_type=f32)
        mixed = mixed + lax.dot_general(low_ref[...], rows, dims, preferred_element_type=f32)
        for i in range(total // share):
            out_ref[i] = mixed[i * share : (i + 1) * share, :].astype(bf16)

    return call(body, [((total // share, share, part), bf16)], [VMEM] * 3)(received, high, low)


def sum_rows(shares, n_dp):
    peers, share, part = shares.shape

    def body(shares_ref, out_ref):
        for d in range(n_dp):
            total = shares_ref[d].astype(f32)
            for z in range(1, peers // n_dp):
                total = total + shares_ref[z * n_dp + d].astype(f32)
            out_ref[:, d * part : (d + 1) * part] = total.astype(bf16)

    return call(body, [((share, n_dp * part), bf16)], [VMEM])(shares)


def exchange(value, axes):
    return lax.all_to_all(value, axes, split_axis=0, concat_axis=0, tiled=True)


def on_device(tokens, expert_ids, route_logits, expert_gate, expert_up, expert_down):
    rows, width = tokens.shape
    top = expert_ids.shape[1]
    n_x, n_pair, n_c, n_dp = (lax.axis_size(a) for a in ("x", "zh", "c", "y"))
    part = width // n_dp
    experts = n_x * 2 * n_c
    held = n_pair * SLOTS
    slots = experts * held
    member = lax.axis_index("y").astype(i32)
    member_ref = member.reshape(1)
    pair_ref = lax.axis_index("zh").astype(i32).reshape(1)
    w_gate, w_up = expert_gate[0], expert_up[0]

    packed = pack_rows(tokens, expert_ids, route_logits, member_ref, n_dp, n_pair)
    gathered = exchange(packed, "zh").reshape(n_pair * rows, -1)

    downs = []
    for s in range(n_dp):
        owner = member + s
        owner = jnp.where(owner >= n_dp, owner - n_dp, owner)
        piece = lax.dynamic_slice_in_dim(expert_down[0], owner * part, part, axis=1)
        if s:
            piece = lax.ppermute(piece, "y", [(i, (i + s) % n_dp) for i in range(n_dp)])
        downs.append(piece)

    ahead, wanted = route_masks(pair_ref, n_pair * rows, rows, held)
    outgoing, high, low = route_rows(gathered, pair_ref, ahead, wanted, top, n_x, n_pair, n_c, n_dp)
    arrived = exchange(outgoing.reshape(n_dp * experts, held, part), ("y", "c", "x", "zl"))
    hidden = hidden_rows(arrived.reshape(n_dp, slots, part), w_gate, w_up)
    hidden, downs = lax.optimization_barrier((hidden, downs))
    hidden = exchange(hidden, "y")
    results = output_rows(hidden, downs, member_ref)
    back = exchange(results.reshape(experts, held, part), ("c", "x", "zl"))
    mixed = mix_rows(back.reshape(slots, part), high, low, rows // n_dp)
    shares = exchange(mixed, ("zh", "y"))
    return sum_rows(shares, n_dp)


def solution(mesh):
    n_ep, n_dp = mesh.devices.shape
    grid = mesh.devices.reshape(CHIPS_X, n_ep // (CHIPS_X * 2 * CORES), 2, CORES, n_dp)
    fine = Mesh(grid, ("x", "zh", "zl", "c", "y"))
    ep = ("x", "zh", "zl", "c")
    placed = (
        P(ep, None),
        P(ep, None),
        P(ep, None),
        P(ep, None, "y"),
        P(ep, None, "y"),
        P(ep, "y", None),
    )
    return jax.shard_map(
        on_device, mesh=fine, in_specs=placed, out_specs=P(ep + ("y",), None), check_vma=False
    )
```

```python
import jax
import jax.numpy as jnp
from jax import lax
from jax.experimental import pallas as pl
from jax.experimental.pallas import tpu as pltpu
from jax.sharding import Mesh, PartitionSpec as P


route_scale = 2.5
SIDE = 128
SLOTS = 4
CHIPS_X, CORES = 4, 2

f32, bf16, i32 = jnp.float32, jnp.bfloat16, jnp.int32
PARAMS = pltpu.CompilerParams(vmem_limit_bytes=20 * 1024 * 1024)
VMEM = pl.BlockSpec(memory_space=pltpu.VMEM)
HBM = pl.BlockSpec(memory_space=pltpu.HBM)
SMEM = pl.BlockSpec(memory_space=pltpu.SMEM)


def call(body, outs, ins, scratch=(), params=PARAMS):
    many = isinstance(outs, tuple)
    return pl.pallas_call(
        body,
        out_shape=tuple(jax.ShapeDtypeStruct(*o) for o in outs) if many else jax.ShapeDtypeStruct(*outs[0]),
        in_specs=ins,
        out_specs=(VMEM,) * len(outs) if many else VMEM,
        scratch_shapes=list(scratch),
        compiler_params=params,
    )


def pack_rows(tokens, expert_ids, route_logits, member, n_dp, peers):
    rows, width = tokens.shape
    top = expert_ids.shape[1]
    part = width // n_dp

    def body(member_ref, tokens_hbm, ids_hbm, logits_hbm, out_ref, own_ref, ids_ref, logits_ref, sems):
        start = pl.multiple_of(member_ref[0] * part, 128)
        copies = [
            pltpu.make_async_copy(tokens_hbm.at[:, pl.ds(start, part)], own_ref, sems.at[0]),
            pltpu.make_async_copy(ids_hbm, ids_ref, sems.at[1]),
            pltpu.make_async_copy(logits_hbm, logits_ref, sems.at[2]),
        ]
        for copy in copies:
            copy.start()
        for copy in copies:
            copy.wait()
        own = own_ref[...]
        scores = 1.0 / (1.0 + jnp.exp(-logits_ref[...]))
        weights = route_scale * scores / jnp.sum(scores, axis=0, keepdims=True)
        high = weights.astype(bf16).astype(f32)
        side = jnp.concatenate(
            [ids_ref[...].astype(f32), high, weights - high, jnp.zeros((SIDE - 3 * top, rows), f32)], axis=0
        )
        side = side.T.astype(bf16)
        for z in range(peers):
            out_ref[z, :, :part] = own
            out_ref[z, :, part:] = side

    outs = [((peers, rows, part + SIDE), bf16)]
    scratch = [
        pltpu.VMEM((rows, part), bf16),
        pltpu.VMEM((top, rows), i32),
        pltpu.VMEM((top, rows), f32),
        pltpu.SemaphoreType.DMA((3,)),
    ]
    return call(body, outs, [SMEM, HBM, HBM, HBM], scratch, None)(member, tokens, expert_ids.T, route_logits.T)


def route_masks(pair, total, rows, held):
    def body(pair_ref, ahead_ref, wanted_ref):
        one = lax.broadcasted_iota(i32, (total, total), 0)
        two = lax.broadcasted_iota(i32, (total, total), 1)
        ahead_ref[...] = jnp.where((one // rows == two // rows) & (one < two), 1.0, 0.0).astype(bf16)
        spot = lax.broadcasted_iota(i32, (held, total), 0)
        token = lax.broadcasted_iota(i32, (held, total), 1)
        wanted_ref[...] = jnp.where(token // rows == spot // SLOTS, spot % SLOTS, -2).astype(f32)

    outs = (((total, total), bf16), ((held, total), f32))
    return call(body, outs, [SMEM])(pair)


def route_rows(gathered, pair, ahead, wanted, top, n_x, n_pair, n_c, n_dp):
    total = gathered.shape[0]
    part = gathered.shape[1] - SIDE
    experts = n_x * 2 * n_c
    held = n_pair * SLOTS
    pad = max(16, experts)

    def body(pair_ref, gathered_ref, ahead_ref, wanted_ref, out_ref, high_ref, low_ref, pick_ref):
        side = gathered_ref[:, part:].astype(f32).T
        line = lax.broadcasted_iota(i32, (pad, 1), 0)
        core, chip, side_plane = line // (2 * n_x), line // 2 % n_x, line % 2
        name = ((chip * n_pair + pair_ref[0]) * 2 + side_plane) * n_c + core
        name = jnp.where(line < experts, name, -1).astype(f32)
        named = jnp.zeros((pad, total), f32)
        high = jnp.zeros((pad, total), f32)
        low = jnp.zeros((pad, total), f32)
        for k in range(top):
            same = side[k : k + 1, :] == name
            named = named + jnp.where(same, 1.0, 0.0)
            high = high + jnp.where(same, side[top + k : top + k + 1, :], 0.0)
            low = low + jnp.where(same, side[2 * top + k : 2 * top + k + 1, :], 0.0)
        rank = jnp.dot(named.astype(bf16), ahead_ref[...], preferred_element_type=f32)
        rank = jnp.where(named > 0.5, rank, -1.0)
        wanted = wanted_ref[...]
        for j in range(experts):
            hit = rank[j : j + 1, :] == wanted
            at = slice(j * held, (j + 1) * held)
            pick_ref[at, :] = jnp.where(hit, 1.0, 0.0).astype(bf16)
            high_ref[at, :] = jnp.where(hit, high[j : j + 1, :], 0.0).astype(bf16)
            low_ref[at, :] = jnp.where(hit, low[j : j + 1, :], 0.0).astype(bf16)
        sent = jnp.dot(pick_ref[...], gathered_ref[:, :part], preferred_element_type=f32).astype(bf16)
        for d in range(n_dp):
            out_ref[d] = sent

    slots = experts * held
    outs = (((n_dp, slots, part), bf16),) + (((slots, total), bf16),) * 2
    scratch = [pltpu.VMEM((slots, total), bf16)]
    return call(body, outs, [SMEM] + [VMEM] * 3, scratch)(pair, gathered, ahead, wanted)


def hidden_rows(received, w_gate, w_up):
    n_dp, slots, part = received.shape
    units = w_gate.shape[1]

    def body(rows_ref, gate_ref, up_ref, out_ref):
        v = jnp.zeros((slots, units), f32)
        u = jnp.zeros((slots, units), f32)
        for d in range(n_dp):
            rows = rows_ref[d]
            at = slice(d * part, (d + 1) * part)
            v = v + jnp.dot(rows, gate_ref[at, :], preferred_element_type=f32)
            u = u + jnp.dot(rows, up_ref[at, :], preferred_element_type=f32)
        out_ref[...] = (v / (1.0 + jnp.exp(-v)) * u).astype(bf16)

    return call(body, [((slots, units), bf16)], [VMEM] * 3)(received, w_gate, w_up)


def output_rows(hiddens, downs):
    count = len(downs)
    slots = hiddens[0].shape[0]
    part = downs[0].shape[1]

    def body(*refs):
        total = jnp.zeros((slots, part), f32)
        for s in range(count):
            total = total + jnp.dot(refs[s][...], refs[count + s][...], preferred_element_type=f32)
        refs[-1][...] = total.astype(bf16)

    return call(body, [((slots, part), bf16)], [VMEM] * (2 * count))(*hiddens, *downs)


def mix_rows(received, high, low, share):
    _, part = received.shape
    total = high.shape[1]

    def body(rows_ref, high_ref, low_ref, out_ref):
        rows = rows_ref[...]
        dims = (((0,), (0,)), ((), ()))
        mixed = lax.dot_general(high_ref[...], rows, dims, preferred_element_type=f32)
        mixed = mixed + lax.dot_general(low_ref[...], rows, dims, preferred_element_type=f32)
        for i in range(total // share):
            out_ref[i] = mixed[i * share : (i + 1) * share, :].astype(bf16)

    return call(body, [((total // share, share, part), bf16)], [VMEM] * 3)(received, high, low)


def sum_rows(shares, n_dp):
    peers, share, part = shares.shape

    def body(shares_ref, out_ref):
        for d in range(n_dp):
            total = shares_ref[d].astype(f32)
            for z in range(1, peers // n_dp):
                total = total + shares_ref[z * n_dp + d].astype(f32)
            out_ref[:, d * part : (d + 1) * part] = total.astype(bf16)

    return call(body, [((share, n_dp * part), bf16)], [VMEM])(shares)


def exchange(value, axes):
    return lax.all_to_all(value, axes, split_axis=0, concat_axis=0, tiled=True)


def on_device(tokens, expert_ids, route_logits, expert_gate, expert_up, expert_down):
    rows, width = tokens.shape
    top = expert_ids.shape[1]
    n_x, n_pair, n_c, n_dp = (lax.axis_size(a) for a in ("x", "zh", "c", "y"))
    part = width // n_dp
    experts = n_x * 2 * n_c
    held = n_pair * SLOTS
    slots = experts * held
    member = lax.axis_index("y").astype(i32)
    member_ref = member.reshape(1)
    pair_ref = lax.axis_index("zh").astype(i32).reshape(1)
    w_gate, w_up = expert_gate[0], expert_up[0]

    packed = pack_rows(tokens, expert_ids, route_logits, member_ref, n_dp, n_pair)
    gathered = exchange(packed, "zh").reshape(n_pair * rows, -1)

    downs = []
    for s in range(n_dp):
        owner = member + s
        owner = jnp.where(owner >= n_dp, owner - n_dp, owner)
        piece = lax.dynamic_slice_in_dim(expert_down[0], owner * part, part, axis=1)
        if s:
            piece = lax.ppermute(piece, "y", [(i, (i + s) % n_dp) for i in range(n_dp)])
        downs.append(piece)

    ahead, wanted = route_masks(pair_ref, n_pair * rows, rows, held)
    outgoing, high, low = route_rows(gathered, pair_ref, ahead, wanted, top, n_x, n_pair, n_c, n_dp)
    arrived = exchange(outgoing.reshape(n_dp * experts, held, part), ("y", "c", "x", "zl"))
    hidden = hidden_rows(arrived.reshape(n_dp, slots, part), w_gate, w_up)
    hidden, downs = lax.optimization_barrier((hidden, downs))
    hiddens = [hidden]
    for s in range(1, n_dp):
        hiddens.append(lax.ppermute(hidden, "y", [(i, (i + s) % n_dp) for i in range(n_dp)]))
    results = output_rows(hiddens, downs)
    back = exchange(results.reshape(experts, held, part), ("c", "x", "zl"))
    mixed = mix_rows(back.reshape(slots, part), high, low, rows // n_dp)
    shares = exchange(mixed, ("zh", "y"))
    return sum_rows(shares, n_dp)


def solution(mesh):
    n_ep, n_dp = mesh.devices.shape
    grid = mesh.devices.reshape(CHIPS_X, n_ep // (CHIPS_X * 2 * CORES), 2, CORES, n_dp)
    fine = Mesh(grid, ("x", "zh", "zl", "c", "y"))
    ep = ("x", "zh", "zl", "c")
    placed = (
        P(ep, None),
        P(ep, None),
        P(ep, None),
        P(ep, None, "y"),
        P(ep, None, "y"),
        P(ep, "y", None),
    )
    return jax.shard_map(
        on_device, mesh=fine, in_specs=placed, out_specs=P(ep + ("y",), None), check_vma=False
    )
```

```python
import jax
import jax.numpy as jnp
from jax import lax
from jax.experimental import pallas as pl
from jax.experimental.pallas import tpu as pltpu
from jax.sharding import Mesh, PartitionSpec as P


route_scale = 2.5
LANES, SIDE = 128, 8
SLOTS = 4
CHIPS_X, CORES = 4, 2

f32, bf16, i32 = jnp.float32, jnp.bfloat16, jnp.int32
PARAMS = pltpu.CompilerParams(vmem_limit_bytes=20 * 1024 * 1024)
VMEM = pl.BlockSpec(memory_space=pltpu.VMEM)
HBM = pl.BlockSpec(memory_space=pltpu.HBM)
SMEM = pl.BlockSpec(memory_space=pltpu.SMEM)


def call(body, outs, ins, scratch=(), params=PARAMS):
    many = isinstance(outs, tuple)
    return pl.pallas_call(
        body,
        out_shape=tuple(jax.ShapeDtypeStruct(*o) for o in outs) if many else jax.ShapeDtypeStruct(*outs[0]),
        in_specs=ins,
        out_specs=(VMEM,) * len(outs) if many else VMEM,
        scratch_shapes=list(scratch),
        compiler_params=params,
    )


def pack_rows(tokens, expert_ids, route_logits, member, n_dp, peers):
    rows, width = tokens.shape
    top = expert_ids.shape[1]
    part = width // n_dp
    pieces = part // LANES

    def body(member_ref, tokens_hbm, ids_hbm, logits_hbm, out_ref, own_ref, ids_ref, logits_ref, sems):
        start = pl.multiple_of(member_ref[0] * part, 128)
        copies = [
            pltpu.make_async_copy(tokens_hbm.at[:, pl.ds(start, part)], own_ref, sems.at[0]),
            pltpu.make_async_copy(ids_hbm, ids_ref, sems.at[1]),
            pltpu.make_async_copy(logits_hbm, logits_ref, sems.at[2]),
        ]
        for copy in copies:
            copy.start()
        for copy in copies:
            copy.wait()
        own = own_ref[...]
        scores = 1.0 / (1.0 + jnp.exp(-logits_ref[...]))
        weights = route_scale * scores / jnp.sum(scores, axis=0, keepdims=True)
        high = weights.astype(bf16).astype(f32)
        side = jnp.concatenate(
            [ids_ref[...].astype(f32), high, weights - high, jnp.zeros((top, LANES - 3 * rows), f32)], axis=1
        )
        if top < SIDE:
            side = jnp.concatenate([side, jnp.zeros((SIDE - top, LANES), f32)], axis=0)
        side = side.astype(bf16)
        for z in range(peers):
            for i in range(pieces):
                out_ref[z, i * rows : (i + 1) * rows, :] = own[:, i * LANES : (i + 1) * LANES]
            out_ref[z, pieces * rows :, :] = side

    outs = [((peers, pieces * rows + SIDE, LANES), bf16)]
    scratch = [
        pltpu.VMEM((rows, part), bf16),
        pltpu.VMEM((top, rows), i32),
        pltpu.VMEM((top, rows), f32),
        pltpu.SemaphoreType.DMA((3,)),
    ]
    return call(body, outs, [SMEM, HBM, HBM, HBM], scratch, None)(member, tokens, expert_ids.T, route_logits.T)


def route_masks(pair, total, rows, held):
    def body(pair_ref, ahead_ref, wanted_ref):
        one = lax.broadcasted_iota(i32, (total, total), 0)
        two = lax.broadcasted_iota(i32, (total, total), 1)
        ahead_ref[...] = jnp.where((one // rows == two // rows) & (one < two), 1.0, 0.0).astype(bf16)
        spot = lax.broadcasted_iota(i32, (held, total), 0)
        token = lax.broadcasted_iota(i32, (held, total), 1)
        wanted_ref[...] = jnp.where(token // rows == spot // SLOTS, spot % SLOTS, -2).astype(f32)

    outs = (((total, total), bf16), ((held, total), f32))
    return call(body, outs, [SMEM])(pair)


def route_rows(gathered, pair, ahead, wanted, rows, top, n_x, n_pair, n_c, n_dp):
    blocks = gathered.shape[0]
    total = blocks * rows
    pieces = (gathered.shape[1] - SIDE) // rows
    part = pieces * LANES
    experts = n_x * 2 * n_c
    held = n_pair * SLOTS
    pad = max(16, experts)

    def body(pair_ref, gathered_ref, ahead_ref, wanted_ref, out_ref, high_ref, low_ref, pick_ref, own_ref):
        for i in range(pieces):
            own_ref[:, i * LANES : (i + 1) * LANES] = gathered_ref[:, i * rows : (i + 1) * rows, :].reshape(total, LANES)
        lane = lax.broadcasted_iota(i32, (SIDE, LANES), 1) // rows
        fields = []
        for f in range(3):
            field = jnp.zeros((SIDE, LANES), f32)
            for b in range(blocks):
                side = gathered_ref[b, pieces * rows :, :].astype(f32)
                if b != f:
                    side = pltpu.roll(side, (b - f) * rows % LANES, 1)
                field = jnp.where(lane == b, side, field)
            fields.append(field[:, :total])
        ids, highs, lows = fields
        line = lax.broadcasted_iota(i32, (pad, 1), 0)
        core, chip, side_plane = line // (2 * n_x), line // 2 % n_x, line % 2
        name = ((chip * n_pair + pair_ref[0]) * 2 + side_plane) * n_c + core
        name = jnp.where(line < experts, name, -1).astype(f32)
        named = jnp.zeros((pad, total), f32)
        high = jnp.zeros((pad, total), f32)
        low = jnp.zeros((pad, total), f32)
        for k in range(top):
            same = ids[k : k + 1, :] == name
            named = named + jnp.where(same, 1.0, 0.0)
            high = high + jnp.where(same, highs[k : k + 1, :], 0.0)
            low = low + jnp.where(same, lows[k : k + 1, :], 0.0)
        rank = jnp.dot(named.astype(bf16), ahead_ref[...], preferred_element_type=f32)
        rank = jnp.where(named > 0.5, rank, -1.0)
        wanted = wanted_ref[...]
        for j in range(experts):
            hit = rank[j : j + 1, :] == wanted
            at = slice(j * held, (j + 1) * held)
            pick_ref[at, :] = jnp.where(hit, 1.0, 0.0).astype(bf16)
            high_ref[at, :] = jnp.where(hit, high[j : j + 1, :], 0.0).astype(bf16)
            low_ref[at, :] = jnp.where(hit, low[j : j + 1, :], 0.0).astype(bf16)
        sent = jnp.dot(pick_ref[...], own_ref[...], preferred_element_type=f32).astype(bf16)
        for d in range(n_dp):
            out_ref[d] = sent

    slots = experts * held
    outs = (((n_dp, slots, part), bf16),) + (((slots, total), bf16),) * 2
    scratch = [pltpu.VMEM((slots, total), bf16), pltpu.VMEM((total, part), bf16)]
    return call(body, outs, [SMEM] + [VMEM] * 3, scratch)(pair, gathered, ahead, wanted)


def hidden_rows(received, w_gate, w_up):
    n_dp, slots, part = received.shape
    units = w_gate.shape[1]

    def body(rows_ref, gate_ref, up_ref, out_ref):
        v = jnp.zeros((slots, units), f32)
        u = jnp.zeros((slots, units), f32)
        for d in range(n_dp):
            rows = rows_ref[d]
            at = slice(d * part, (d + 1) * part)
            v = v + jnp.dot(rows, gate_ref[at, :], preferred_element_type=f32)
            u = u + jnp.dot(rows, up_ref[at, :], preferred_element_type=f32)
        made = (v / (1.0 + jnp.exp(-v)) * u).astype(bf16)
        for d in range(n_dp):
            out_ref[d] = made

    return call(body, [((n_dp, slots, units), bf16)], [VMEM] * 3)(received, w_gate, w_up)


def output_rows(hidden, downs, member):
    n_dp, slots, _ = hidden.shape
    part = downs[0].shape[1]

    def body(member_ref, hidden_ref, *refs):
        out_ref = refs[-1]
        total = jnp.zeros((slots, part), f32)
        for s in range(n_dp):
            source = lax.rem(member_ref[0] + (n_dp - s), n_dp)
            total = total + jnp.dot(hidden_ref[source], refs[s][...], preferred_element_type=f32)
        out_ref[...] = total.astype(bf16)

    return call(body, [((slots, part), bf16)], [SMEM, VMEM] + [VMEM] * n_dp)(
        member, hidden, *downs
    )


def mix_rows(received, high, low, share, n_dp):
    _, part = received.shape
    total = high.shape[1]

    def body(rows_ref, high_ref, low_ref, out_ref):
        rows = rows_ref[...]
        dims = (((0,), (0,)), ((), ()))
        mixed = lax.dot_general(high_ref[...], rows, dims, preferred_element_type=f32)
        mixed = mixed + lax.dot_general(low_ref[...], rows, dims, preferred_element_type=f32)
        for i in range(total // share):
            block, owner = i // n_dp, i % n_dp
            out_ref[owner * (total // share // n_dp) + block] = mixed[i * share : (i + 1) * share, :].astype(bf16)

    return call(body, [((total // share, share, part), bf16)], [VMEM] * 3)(received, high, low)


def sum_rows(shares, n_dp):
    peers, share, part = shares.shape

    def body(shares_ref, out_ref):
        for d in range(n_dp):
            first = d * (peers // n_dp)
            total = shares_ref[first].astype(f32)
            for z in range(1, peers // n_dp):
                total = total + shares_ref[first + z].astype(f32)
            out_ref[:, d * part : (d + 1) * part] = total.astype(bf16)

    return call(body, [((share, n_dp * part), bf16)], [VMEM])(shares)


def exchange(value, axes):
    return lax.all_to_all(value, axes, split_axis=0, concat_axis=0, tiled=True)


def on_device(tokens, expert_ids, route_logits, expert_gate, expert_up, expert_down):
    rows, width = tokens.shape
    top = expert_ids.shape[1]
    n_x, n_pair, n_c, n_dp = (lax.axis_size(a) for a in ("x", "zh", "c", "y"))
    part = width // n_dp
    experts = n_x * 2 * n_c
    held = n_pair * SLOTS
    slots = experts * held
    member = lax.axis_index("y").astype(i32)
    member_ref = member.reshape(1)
    pair_ref = lax.axis_index("zh").astype(i32).reshape(1)
    w_gate, w_up = expert_gate[0], expert_up[0]

    packed = pack_rows(tokens, expert_ids, route_logits, member_ref, n_dp, n_pair)
    gathered = exchange(packed, "zh")

    downs = []
    for s in range(n_dp):
        owner = member + s
        owner = jnp.where(owner >= n_dp, owner - n_dp, owner)
        piece = lax.dynamic_slice_in_dim(expert_down[0], owner * part, part, axis=1)
        if s:
            piece = lax.ppermute(piece, "y", [(i, (i + s) % n_dp) for i in range(n_dp)])
        downs.append(piece)

    ahead, wanted = route_masks(pair_ref, n_pair * rows, rows, held)
    outgoing, high, low = route_rows(
        gathered, pair_ref, ahead, wanted, rows, top, n_x, n_pair, n_c, n_dp
    )
    arrived = exchange(outgoing.reshape(n_dp * experts, held, part), ("y", "c", "x", "zl"))
    hidden = hidden_rows(arrived.reshape(n_dp, slots, part), w_gate, w_up)
    hidden, downs = lax.optimization_barrier((hidden, downs))
    hidden = exchange(hidden, "y")
    results = output_rows(hidden, downs, member_ref)
    back = exchange(results.reshape(experts, held, part), ("c", "x", "zl"))
    mixed = mix_rows(back.reshape(slots, part), high, low, rows // n_dp, n_dp)
    shares = exchange(mixed, ("y", "zh"))
    return sum_rows(shares, n_dp)


def solution(mesh):
    n_ep, n_dp = mesh.devices.shape
    grid = mesh.devices.reshape(CHIPS_X, n_ep // (CHIPS_X * 2 * CORES), 2, CORES, n_dp)
    fine = Mesh(grid, ("x", "zh", "zl", "c", "y"))
    ep = ("x", "zh", "zl", "c")
    placed = (
        P(ep, None),
        P(ep, None),
        P(ep, None),
        P(ep, None, "y"),
        P(ep, None, "y"),
        P(ep, "y", None),
    )
    return jax.shard_map(
        on_device, mesh=fine, in_specs=placed, out_specs=P(ep + ("y",), None), check_vma=False
    )
```

```python
import jax
import jax.numpy as jnp
from jax import lax
from jax.experimental import pallas as pl
from jax.experimental.pallas import tpu as pltpu
from jax.sharding import Mesh, PartitionSpec as P


route_scale = 2.5
LANES, SIDE = 128, 8
SLOTS = 4
CHIPS_X, CORES = 4, 2

f32, bf16, i32 = jnp.float32, jnp.bfloat16, jnp.int32
PARAMS = pltpu.CompilerParams(vmem_limit_bytes=20 * 1024 * 1024)
VMEM = pl.BlockSpec(memory_space=pltpu.VMEM)
HBM = pl.BlockSpec(memory_space=pltpu.HBM)
SMEM = pl.BlockSpec(memory_space=pltpu.SMEM)


def call(body, outs, ins, scratch=(), params=PARAMS):
    many = isinstance(outs, tuple)
    return pl.pallas_call(
        body,
        out_shape=tuple(jax.ShapeDtypeStruct(*o) for o in outs) if many else jax.ShapeDtypeStruct(*outs[0]),
        in_specs=ins,
        out_specs=(VMEM,) * len(outs) if many else VMEM,
        scratch_shapes=list(scratch),
        compiler_params=params,
    )


def pack_rows(tokens, expert_ids, route_logits, member, n_dp, peers):
    rows, width = tokens.shape
    top = expert_ids.shape[1]
    part = width // n_dp
    pieces = part // LANES

    def body(member_ref, tokens_hbm, ids_hbm, logits_hbm, out_ref, own_ref, ids_ref, logits_ref, sems):
        start = pl.multiple_of(member_ref[0] * part, 128)
        copies = [
            pltpu.make_async_copy(tokens_hbm.at[:, pl.ds(start, part)], own_ref, sems.at[0]),
            pltpu.make_async_copy(ids_hbm, ids_ref, sems.at[1]),
            pltpu.make_async_copy(logits_hbm, logits_ref, sems.at[2]),
        ]
        for copy in copies:
            copy.start()
        for copy in copies:
            copy.wait()
        own = own_ref[...]
        scores = 1.0 / (1.0 + jnp.exp(-logits_ref[...]))
        weights = route_scale * scores / jnp.sum(scores, axis=0, keepdims=True)
        high = weights.astype(bf16).astype(f32)
        side = jnp.concatenate(
            [ids_ref[...].astype(f32), high, weights - high, jnp.zeros((top, LANES - 3 * rows), f32)], axis=1
        )
        if top < SIDE:
            side = jnp.concatenate([side, jnp.zeros((SIDE - top, LANES), f32)], axis=0)
        side = side.astype(bf16)
        for z in range(peers):
            for i in range(pieces):
                out_ref[z, i * rows : (i + 1) * rows, :] = own[:, i * LANES : (i + 1) * LANES]
            out_ref[z, pieces * rows :, :] = side

    outs = [((peers, pieces * rows + SIDE, LANES), bf16)]
    scratch = [
        pltpu.VMEM((rows, part), bf16),
        pltpu.VMEM((top, rows), i32),
        pltpu.VMEM((top, rows), f32),
        pltpu.SemaphoreType.DMA((3,)),
    ]
    return call(body, outs, [SMEM, HBM, HBM, HBM], scratch, None)(member, tokens, expert_ids.T, route_logits.T)


def route_masks(pair, total, rows, held):
    def body(pair_ref, ahead_ref, wanted_ref):
        one = lax.broadcasted_iota(i32, (total, total), 0)
        two = lax.broadcasted_iota(i32, (total, total), 1)
        ahead_ref[...] = jnp.where((one // rows == two // rows) & (one < two), 1.0, 0.0).astype(bf16)
        spot = lax.broadcasted_iota(i32, (held, total), 0)
        token = lax.broadcasted_iota(i32, (held, total), 1)
        wanted_ref[...] = jnp.where(token // rows == spot // SLOTS, spot % SLOTS, -2).astype(f32)

    outs = (((total, total), bf16), ((held, total), f32))
    return call(body, outs, [SMEM])(pair)


def route_rows(gathered, pair, ahead, wanted, rows, top, n_x, n_pair, n_c, n_dp):
    blocks = gathered.shape[0]
    total = blocks * rows
    pieces = (gathered.shape[1] - SIDE) // rows
    part = pieces * LANES
    experts = n_x * 2 * n_c
    held = n_pair * SLOTS
    pad = max(16, experts)

    def body(pair_ref, gathered_ref, ahead_ref, wanted_ref, out_ref, high_ref, low_ref, pick_ref, own_ref):
        for i in range(pieces):
            own_ref[:, i * LANES : (i + 1) * LANES] = gathered_ref[:, i * rows : (i + 1) * rows, :].reshape(total, LANES)
        lane = lax.broadcasted_iota(i32, (SIDE, LANES), 1) // rows
        fields = []
        for f in range(3):
            field = jnp.zeros((SIDE, LANES), f32)
            for b in range(blocks):
                side = gathered_ref[b, pieces * rows :, :].astype(f32)
                if b != f:
                    side = pltpu.roll(side, (b - f) * rows % LANES, 1)
                field = jnp.where(lane == b, side, field)
            fields.append(field[:, :total])
        ids, highs, lows = fields
        line = lax.broadcasted_iota(i32, (pad, 1), 0)
        core, chip, side_plane = line // (2 * n_x), line // 2 % n_x, line % 2
        name = ((chip * n_pair + pair_ref[0]) * 2 + side_plane) * n_c + core
        name = jnp.where(line < experts, name, -1).astype(f32)
        named = jnp.zeros((pad, total), f32)
        high = jnp.zeros((pad, total), f32)
        low = jnp.zeros((pad, total), f32)
        for k in range(top):
            same = ids[k : k + 1, :] == name
            named = named + jnp.where(same, 1.0, 0.0)
            high = high + jnp.where(same, highs[k : k + 1, :], 0.0)
            low = low + jnp.where(same, lows[k : k + 1, :], 0.0)
        rank = jnp.dot(named.astype(bf16), ahead_ref[...], preferred_element_type=f32)
        rank = jnp.where(named > 0.5, rank, -1.0)
        wanted = wanted_ref[...]
        for j in range(experts):
            hit = rank[j : j + 1, :] == wanted
            at = slice(j * held, (j + 1) * held)
            pick_ref[at, :] = jnp.where(hit, 1.0, 0.0).astype(bf16)
            high_ref[at, :] = jnp.where(hit, high[j : j + 1, :], 0.0).astype(bf16)
            low_ref[at, :] = jnp.where(hit, low[j : j + 1, :], 0.0).astype(bf16)
        sent = jnp.dot(pick_ref[...], own_ref[...], preferred_element_type=f32).astype(bf16)
        for d in range(n_dp):
            out_ref[d] = sent

    slots = experts * held
    outs = (((n_dp, slots, part), bf16),) + (((slots, total), bf16),) * 2
    scratch = [pltpu.VMEM((slots, total), bf16), pltpu.VMEM((total, part), bf16)]
    return call(body, outs, [SMEM] + [VMEM] * 3, scratch)(pair, gathered, ahead, wanted)


def hidden_rows(received, w_gate, w_up):
    n_dp, slots, part = received.shape
    units = w_gate.shape[1]

    def body(rows_ref, gate_ref, up_ref, out_ref):
        v = jnp.zeros((slots, units), f32)
        u = jnp.zeros((slots, units), f32)
        for d in range(n_dp):
            rows = rows_ref[d]
            at = slice(d * part, (d + 1) * part)
            v = v + jnp.dot(rows, gate_ref[at, :], preferred_element_type=f32)
            u = u + jnp.dot(rows, up_ref[at, :], preferred_element_type=f32)
        made = (v / (1.0 + jnp.exp(-v)) * u).astype(bf16)
        for d in range(n_dp):
            out_ref[d] = made

    return call(body, [((n_dp, slots, units), bf16)], [VMEM] * 3)(received, w_gate, w_up)


def output_rows(hidden, down, downs, member):
    n_dp, slots, _ = hidden.shape
    part = downs[0].shape[1]

    def body(member_ref, hidden_ref, down_ref, *refs):
        start = pl.multiple_of(member_ref[0] * part, 128)
        total = jnp.dot(hidden_ref[member_ref[0]], down_ref[:, pl.ds(start, part)], preferred_element_type=f32)
        for s in range(1, n_dp):
            source = lax.rem(member_ref[0] + (n_dp - s), n_dp)
            total = total + jnp.dot(hidden_ref[source], refs[s - 1][...], preferred_element_type=f32)
        refs[-1][...] = total.astype(bf16)

    return call(body, [((slots, part), bf16)], [SMEM] + [VMEM] * (n_dp + 1))(member, hidden, down, *downs)


def mix_rows(received, high, low, share, n_dp):
    _, part = received.shape
    total = high.shape[1]

    def body(rows_ref, high_ref, low_ref, out_ref):
        rows = rows_ref[...]
        dims = (((0,), (0,)), ((), ()))
        mixed = lax.dot_general(high_ref[...], rows, dims, preferred_element_type=f32)
        mixed = mixed + lax.dot_general(low_ref[...], rows, dims, preferred_element_type=f32)
        for i in range(total // share):
            block, owner = i // n_dp, i % n_dp
            out_ref[owner * (total // share // n_dp) + block] = mixed[i * share : (i + 1) * share, :].astype(bf16)

    return call(body, [((total // share, share, part), bf16)], [VMEM] * 3)(received, high, low)


def sum_rows(shares, n_dp):
    peers, share, part = shares.shape

    def body(shares_ref, out_ref):
        for d in range(n_dp):
            first = d * (peers // n_dp)
            total = shares_ref[first].astype(f32)
            for z in range(1, peers // n_dp):
                total = total + shares_ref[first + z].astype(f32)
            out_ref[:, d * part : (d + 1) * part] = total.astype(bf16)

    return call(body, [((share, n_dp * part), bf16)], [VMEM])(shares)


def exchange(value, axes):
    return lax.all_to_all(value, axes, split_axis=0, concat_axis=0, tiled=True)


def on_device(tokens, expert_ids, route_logits, expert_gate, expert_up, expert_down):
    rows, width = tokens.shape
    top = expert_ids.shape[1]
    n_x, n_pair, n_c, n_dp = (lax.axis_size(a) for a in ("x", "zh", "c", "y"))
    part = width // n_dp
    experts = n_x * 2 * n_c
    held = n_pair * SLOTS
    slots = experts * held
    member = lax.axis_index("y").astype(i32)
    member_ref = member.reshape(1)
    pair_ref = lax.axis_index("zh").astype(i32).reshape(1)
    w_gate, w_up = expert_gate[0], expert_up[0]

    packed = pack_rows(tokens, expert_ids, route_logits, member_ref, n_dp, n_pair)
    gathered = exchange(packed, "zh")

    downs = []
    for s in range(1, n_dp):
        owner = member + s
        owner = jnp.where(owner >= n_dp, owner - n_dp, owner)
        piece = lax.dynamic_slice_in_dim(expert_down[0], owner * part, part, axis=1)
        piece = lax.ppermute(piece, "y", [(i, (i + s) % n_dp) for i in range(n_dp)])
        downs.append(piece)

    ahead, wanted = route_masks(pair_ref, n_pair * rows, rows, held)
    outgoing, high, low = route_rows(
        gathered, pair_ref, ahead, wanted, rows, top, n_x, n_pair, n_c, n_dp
    )
    arrived = exchange(outgoing.reshape(n_dp * experts, held, part), ("y", "c", "x", "zl"))
    hidden = hidden_rows(arrived.reshape(n_dp, slots, part), w_gate, w_up)
    hidden, downs = lax.optimization_barrier((hidden, downs))
    hidden = exchange(hidden, "y")
    results = output_rows(hidden, expert_down[0], downs, member_ref)
    back = exchange(results.reshape(experts, held, part), ("c", "x", "zl"))
    mixed = mix_rows(back.reshape(slots, part), high, low, rows // n_dp, n_dp)
    shares = exchange(mixed, ("y", "zh"))
    return sum_rows(shares, n_dp)


def solution(mesh):
    n_ep, n_dp = mesh.devices.shape
    grid = mesh.devices.reshape(CHIPS_X, n_ep // (CHIPS_X * 2 * CORES), 2, CORES, n_dp)
    fine = Mesh(grid, ("x", "zh", "zl", "c", "y"))
    ep = ("x", "zh", "zl", "c")
    placed = (
        P(ep, None),
        P(ep, None),
        P(ep, None),
        P(ep, None, "y"),
        P(ep, None, "y"),
        P(ep, "y", None),
    )
    return jax.shard_map(
        on_device, mesh=fine, in_specs=placed, out_specs=P(ep + ("y",), None), check_vma=False
    )
```

```python
import jax
import jax.numpy as jnp
from jax import lax
from jax.experimental import pallas as pl
from jax.experimental.pallas import tpu as pltpu
from jax.sharding import Mesh, PartitionSpec as P


route_scale = 2.5
LANES, SIDE = 128, 8
SLOTS = 4
CHIPS_X, CORES = 4, 2

f32, bf16, i32 = jnp.float32, jnp.bfloat16, jnp.int32
PARAMS = pltpu.CompilerParams(vmem_limit_bytes=20 * 1024 * 1024)
VMEM = pl.BlockSpec(memory_space=pltpu.VMEM)
HBM = pl.BlockSpec(memory_space=pltpu.HBM)
SMEM = pl.BlockSpec(memory_space=pltpu.SMEM)


def call(body, outs, ins, scratch=(), params=PARAMS):
    many = isinstance(outs, tuple)
    return pl.pallas_call(
        body,
        out_shape=tuple(jax.ShapeDtypeStruct(*o) for o in outs) if many else jax.ShapeDtypeStruct(*outs[0]),
        in_specs=ins,
        out_specs=(VMEM,) * len(outs) if many else VMEM,
        scratch_shapes=list(scratch),
        compiler_params=params,
    )


def pack_rows(tokens, expert_ids, route_logits, down, member, n_dp, peers):
    rows, width = tokens.shape
    top = expert_ids.shape[1]
    part = width // n_dp
    pieces = part // LANES

    def body(member_ref, tokens_hbm, ids_hbm, logits_hbm, down_hbm, out_ref, *refs):
        pieces_out, (own_ref, ids_ref, logits_ref, sems) = refs[: n_dp - 1], refs[n_dp - 1 :]
        start = pl.multiple_of(member_ref[0] * part, 128)
        copies = [
            pltpu.make_async_copy(tokens_hbm.at[:, pl.ds(start, part)], own_ref, sems.at[0]),
            pltpu.make_async_copy(ids_hbm, ids_ref, sems.at[1]),
            pltpu.make_async_copy(logits_hbm, logits_ref, sems.at[2]),
        ]
        cuts = []
        for s in range(1, n_dp):
            begin = pl.multiple_of(lax.rem(member_ref[0] + s, n_dp) * part, 128)
            cuts.append(
                pltpu.make_async_copy(down_hbm.at[:, pl.ds(begin, part)], pieces_out[s - 1], sems.at[2 + s])
            )
        for copy in copies + cuts:
            copy.start()
        for copy in copies:
            copy.wait()
        own = own_ref[...]
        scores = 1.0 / (1.0 + jnp.exp(-logits_ref[...]))
        weights = route_scale * scores / jnp.sum(scores, axis=0, keepdims=True)
        high = weights.astype(bf16).astype(f32)
        side = jnp.concatenate(
            [ids_ref[...].astype(f32), high, weights - high, jnp.zeros((top, LANES - 3 * rows), f32)], axis=1
        )
        if top < SIDE:
            side = jnp.concatenate([side, jnp.zeros((SIDE - top, LANES), f32)], axis=0)
        side = side.astype(bf16)
        for z in range(peers):
            for i in range(pieces):
                out_ref[z, i * rows : (i + 1) * rows, :] = own[:, i * LANES : (i + 1) * LANES]
            out_ref[z, pieces * rows :, :] = side
        for copy in cuts:
            copy.wait()

    outs = (((peers, pieces * rows + SIDE, LANES), bf16),) + (((down.shape[0], part), bf16),) * (n_dp - 1)
    scratch = [
        pltpu.VMEM((rows, part), bf16),
        pltpu.VMEM((top, rows), i32),
        pltpu.VMEM((top, rows), f32),
        pltpu.SemaphoreType.DMA((2 + n_dp,)),
    ]
    return call(body, outs, [SMEM, HBM, HBM, HBM, HBM], scratch, None)(
        member, tokens, expert_ids.T, route_logits.T, down
    )


def route_masks(pair, total, rows, held):
    def body(pair_ref, ahead_ref, wanted_ref):
        one = lax.broadcasted_iota(i32, (total, total), 0)
        two = lax.broadcasted_iota(i32, (total, total), 1)
        ahead_ref[...] = jnp.where((one // rows == two // rows) & (one < two), 1.0, 0.0).astype(bf16)
        spot = lax.broadcasted_iota(i32, (held, total), 0)
        token = lax.broadcasted_iota(i32, (held, total), 1)
        wanted_ref[...] = jnp.where(token // rows == spot // SLOTS, spot % SLOTS, -2).astype(f32)

    outs = (((total, total), bf16), ((held, total), f32))
    return call(body, outs, [SMEM])(pair)


def route_rows(gathered, pair, ahead, wanted, rows, top, n_x, n_pair, n_c, n_dp):
    blocks = gathered.shape[0]
    total = blocks * rows
    pieces = (gathered.shape[1] - SIDE) // rows
    part = pieces * LANES
    experts = n_x * 2 * n_c
    held = n_pair * SLOTS
    pad = max(16, experts)

    def body(pair_ref, gathered_ref, ahead_ref, wanted_ref, out_ref, high_ref, low_ref, pick_ref, own_ref):
        for i in range(pieces):
            own_ref[:, i * LANES : (i + 1) * LANES] = gathered_ref[:, i * rows : (i + 1) * rows, :].reshape(total, LANES)
        lane = lax.broadcasted_iota(i32, (SIDE, LANES), 1) // rows
        fields = []
        for f in range(3):
            field = jnp.zeros((SIDE, LANES), f32)
            for b in range(blocks):
                side = gathered_ref[b, pieces * rows :, :].astype(f32)
                if b != f:
                    side = pltpu.roll(side, (b - f) * rows % LANES, 1)
                field = jnp.where(lane == b, side, field)
            fields.append(field[:, :total])
        ids, highs, lows = fields
        line = lax.broadcasted_iota(i32, (pad, 1), 0)
        core, chip, side_plane = line // (2 * n_x), line // 2 % n_x, line % 2
        name = ((chip * n_pair + pair_ref[0]) * 2 + side_plane) * n_c + core
        name = jnp.where(line < experts, name, -1).astype(f32)
        named = jnp.zeros((pad, total), f32)
        high = jnp.zeros((pad, total), f32)
        low = jnp.zeros((pad, total), f32)
        for k in range(top):
            same = ids[k : k + 1, :] == name
            named = named + jnp.where(same, 1.0, 0.0)
            high = high + jnp.where(same, highs[k : k + 1, :], 0.0)
            low = low + jnp.where(same, lows[k : k + 1, :], 0.0)
        rank = jnp.dot(named.astype(bf16), ahead_ref[...], preferred_element_type=f32)
        rank = jnp.where(named > 0.5, rank, -1.0)
        wanted = wanted_ref[...]
        for j in range(experts):
            hit = rank[j : j + 1, :] == wanted
            at = slice(j * held, (j + 1) * held)
            pick_ref[at, :] = jnp.where(hit, 1.0, 0.0).astype(bf16)
            high_ref[at, :] = jnp.where(hit, high[j : j + 1, :], 0.0).astype(bf16)
            low_ref[at, :] = jnp.where(hit, low[j : j + 1, :], 0.0).astype(bf16)
        sent = jnp.dot(pick_ref[...], own_ref[...], preferred_element_type=f32).astype(bf16)
        for d in range(n_dp):
            out_ref[d] = sent

    slots = experts * held
    outs = (((n_dp, slots, part), bf16),) + (((slots, total), bf16),) * 2
    scratch = [pltpu.VMEM((slots, total), bf16), pltpu.VMEM((total, part), bf16)]
    return call(body, outs, [SMEM] + [VMEM] * 3, scratch)(pair, gathered, ahead, wanted)


def hidden_rows(received, w_gate, w_up):
    n_dp, slots, part = received.shape
    units = w_gate.shape[1]

    def body(rows_ref, gate_ref, up_ref, out_ref):
        v = jnp.zeros((slots, units), f32)
        u = jnp.zeros((slots, units), f32)
        for d in range(n_dp):
            rows = rows_ref[d]
            at = slice(d * part, (d + 1) * part)
            v = v + jnp.dot(rows, gate_ref[at, :], preferred_element_type=f32)
            u = u + jnp.dot(rows, up_ref[at, :], preferred_element_type=f32)
        made = (v / (1.0 + jnp.exp(-v)) * u).astype(bf16)
        for d in range(n_dp):
            out_ref[d] = made

    return call(body, [((n_dp, slots, units), bf16)], [VMEM] * 3)(received, w_gate, w_up)


def output_rows(hidden, down, downs, member):
    n_dp, slots, _ = hidden.shape
    part = downs[0].shape[1]

    def body(member_ref, hidden_ref, down_ref, *refs):
        start = pl.multiple_of(member_ref[0] * part, 128)
        total = jnp.dot(hidden_ref[member_ref[0]], down_ref[:, pl.ds(start, part)], preferred_element_type=f32)
        for s in range(1, n_dp):
            source = lax.rem(member_ref[0] + (n_dp - s), n_dp)
            total = total + jnp.dot(hidden_ref[source], refs[s - 1][...], preferred_element_type=f32)
        refs[-1][...] = total.astype(bf16)

    return call(body, [((slots, part), bf16)], [SMEM] + [VMEM] * (n_dp + 1))(member, hidden, down, *downs)


def mix_rows(received, high, low, share, n_dp):
    _, part = received.shape
    total = high.shape[1]

    def body(rows_ref, high_ref, low_ref, out_ref):
        rows = rows_ref[...]
        dims = (((0,), (0,)), ((), ()))
        mixed = lax.dot_general(high_ref[...], rows, dims, preferred_element_type=f32)
        mixed = mixed + lax.dot_general(low_ref[...], rows, dims, preferred_element_type=f32)
        for i in range(total // share):
            block, owner = i // n_dp, i % n_dp
            out_ref[owner * (total // share // n_dp) + block] = mixed[i * share : (i + 1) * share, :].astype(bf16)

    return call(body, [((total // share, share, part), bf16)], [VMEM] * 3)(received, high, low)


def sum_rows(shares, n_dp):
    peers, share, part = shares.shape

    def body(shares_ref, out_ref):
        for d in range(n_dp):
            first = d * (peers // n_dp)
            total = shares_ref[first].astype(f32)
            for z in range(1, peers // n_dp):
                total = total + shares_ref[first + z].astype(f32)
            out_ref[:, d * part : (d + 1) * part] = total.astype(bf16)

    return call(body, [((share, n_dp * part), bf16)], [VMEM])(shares)


def exchange(value, axes):
    return lax.all_to_all(value, axes, split_axis=0, concat_axis=0, tiled=True)


def on_device(tokens, expert_ids, route_logits, expert_gate, expert_up, expert_down):
    rows, width = tokens.shape
    top = expert_ids.shape[1]
    n_x, n_pair, n_c, n_dp = (lax.axis_size(a) for a in ("x", "zh", "c", "y"))
    part = width // n_dp
    experts = n_x * 2 * n_c
    held = n_pair * SLOTS
    slots = experts * held
    member = lax.axis_index("y").astype(i32)
    member_ref = member.reshape(1)
    pair_ref = lax.axis_index("zh").astype(i32).reshape(1)
    w_gate, w_up = expert_gate[0], expert_up[0]

    packed, *cuts = pack_rows(
        tokens, expert_ids, route_logits, expert_down[0], member_ref, n_dp, n_pair
    )
    gathered = exchange(packed, "zh")

    downs = []
    for s in range(1, n_dp):
        piece = lax.ppermute(cuts[s - 1], "y", [(i, (i + s) % n_dp) for i in range(n_dp)])
        downs.append(piece)

    ahead, wanted = route_masks(pair_ref, n_pair * rows, rows, held)
    outgoing, high, low = route_rows(
        gathered, pair_ref, ahead, wanted, rows, top, n_x, n_pair, n_c, n_dp
    )
    arrived = exchange(outgoing.reshape(n_dp * experts, held, part), ("y", "c", "x", "zl"))
    hidden = hidden_rows(arrived.reshape(n_dp, slots, part), w_gate, w_up)
    hidden, downs = lax.optimization_barrier((hidden, downs))
    hidden = exchange(hidden, "y")
    results = output_rows(hidden, expert_down[0], downs, member_ref)
    back = exchange(results.reshape(experts, held, part), ("c", "x", "zl"))
    mixed = mix_rows(back.reshape(slots, part), high, low, rows // n_dp, n_dp)
    shares = exchange(mixed, ("y", "zh"))
    return sum_rows(shares, n_dp)


def solution(mesh):
    n_ep, n_dp = mesh.devices.shape
    grid = mesh.devices.reshape(CHIPS_X, n_ep // (CHIPS_X * 2 * CORES), 2, CORES, n_dp)
    fine = Mesh(grid, ("x", "zh", "zl", "c", "y"))
    ep = ("x", "zh", "zl", "c")
    placed = (
        P(ep, None),
        P(ep, None),
        P(ep, None),
        P(ep, None, "y"),
        P(ep, None, "y"),
        P(ep, "y", None),
    )
    return jax.shard_map(
        on_device, mesh=fine, in_specs=placed, out_specs=P(ep + ("y",), None), check_vma=False
    )
```

```python
import jax
import jax.numpy as jnp
from jax import lax
from jax.experimental import pallas as pl
from jax.experimental.pallas import tpu as pltpu
from jax.sharding import Mesh, PartitionSpec as P


route_scale = 2.5
LANES, SIDE = 128, 8
SLOTS = 4
CHIPS_X, CORES = 4, 2

f32, bf16, i32 = jnp.float32, jnp.bfloat16, jnp.int32
PARAMS = pltpu.CompilerParams(vmem_limit_bytes=20 * 1024 * 1024)
VMEM = pl.BlockSpec(memory_space=pltpu.VMEM)
HBM = pl.BlockSpec(memory_space=pltpu.HBM)
SMEM = pl.BlockSpec(memory_space=pltpu.SMEM)


def call(body, outs, ins, scratch=(), params=PARAMS):
    many = isinstance(outs, tuple)
    return pl.pallas_call(
        body,
        out_shape=tuple(jax.ShapeDtypeStruct(*o) for o in outs) if many else jax.ShapeDtypeStruct(*outs[0]),
        in_specs=ins,
        out_specs=(VMEM,) * len(outs) if many else VMEM,
        scratch_shapes=list(scratch),
        compiler_params=params,
    )


def pack_rows(tokens, expert_ids, route_logits, member, n_dp, peers):
    rows, width = tokens.shape
    top = expert_ids.shape[1]
    part = width // n_dp
    pieces = part // LANES

    def body(member_ref, tokens_hbm, ids_hbm, logits_hbm, out_ref, own_ref, ids_ref, logits_ref, sems):
        start = pl.multiple_of(member_ref[0] * part, 128)
        copies = [
            pltpu.make_async_copy(tokens_hbm.at[:, pl.ds(start, part)], own_ref, sems.at[0]),
            pltpu.make_async_copy(ids_hbm, ids_ref, sems.at[1]),
            pltpu.make_async_copy(logits_hbm, logits_ref, sems.at[2]),
        ]
        for copy in copies:
            copy.start()
        for copy in copies:
            copy.wait()
        own = own_ref[...]
        scores = 1.0 / (1.0 + jnp.exp(-logits_ref[...]))
        weights = route_scale * scores / jnp.sum(scores, axis=0, keepdims=True)
        high = weights.astype(bf16).astype(f32)
        side = jnp.concatenate(
            [ids_ref[...].astype(f32), high, weights - high, jnp.zeros((top, LANES - 3 * rows), f32)], axis=1
        )
        if top < SIDE:
            side = jnp.concatenate([side, jnp.zeros((SIDE - top, LANES), f32)], axis=0)
        side = side.astype(bf16)
        for z in range(peers):
            for i in range(pieces):
                out_ref[z, i * rows : (i + 1) * rows, :] = own[:, i * LANES : (i + 1) * LANES]
            out_ref[z, pieces * rows :, :] = side

    outs = [((peers, pieces * rows + SIDE, LANES), bf16)]
    scratch = [
        pltpu.VMEM((rows, part), bf16),
        pltpu.VMEM((top, rows), i32),
        pltpu.VMEM((top, rows), f32),
        pltpu.SemaphoreType.DMA((3,)),
    ]
    return call(body, outs, [SMEM, HBM, HBM, HBM], scratch, None)(member, tokens, expert_ids.T, route_logits.T)


def route_masks(pair, total, rows, held):
    def body(pair_ref, ahead_ref, wanted_ref):
        one = lax.broadcasted_iota(i32, (total, total), 0)
        two = lax.broadcasted_iota(i32, (total, total), 1)
        ahead_ref[...] = jnp.where((one // rows == two // rows) & (one < two), 1.0, 0.0).astype(bf16)
        spot = lax.broadcasted_iota(i32, (held, total), 0)
        token = lax.broadcasted_iota(i32, (held, total), 1)
        wanted_ref[...] = jnp.where(token // rows == spot // SLOTS, spot % SLOTS, -2).astype(f32)

    outs = (((total, total), bf16), ((held, total), f32))
    return call(body, outs, [SMEM])(pair)


def route_rows(gathered, pair, ahead, wanted, rows, top, n_x, n_pair, n_c, n_dp):
    blocks = gathered.shape[0]
    total = blocks * rows
    pieces = (gathered.shape[1] - SIDE) // rows
    part = pieces * LANES
    experts = n_x * 2 * n_c
    held = n_pair * SLOTS
    pad = max(16, experts)

    def body(pair_ref, gathered_ref, ahead_ref, wanted_ref, out_ref, high_ref, low_ref, pick_ref, own_ref):
        for i in range(pieces):
            own_ref[:, i * LANES : (i + 1) * LANES] = gathered_ref[:, i * rows : (i + 1) * rows, :].reshape(total, LANES)
        lane = lax.broadcasted_iota(i32, (SIDE, LANES), 1) // rows
        fields = []
        for f in range(3):
            field = jnp.zeros((SIDE, LANES), f32)
            for b in range(blocks):
                side = gathered_ref[b, pieces * rows :, :].astype(f32)
                if b != f:
                    side = pltpu.roll(side, (b - f) * rows % LANES, 1)
                field = jnp.where(lane == b, side, field)
            fields.append(field[:, :total])
        ids, highs, lows = fields
        line = lax.broadcasted_iota(i32, (pad, 1), 0)
        core, chip, side_plane = line // (2 * n_x), line // 2 % n_x, line % 2
        name = ((chip * n_pair + pair_ref[0]) * 2 + side_plane) * n_c + core
        name = jnp.where(line < experts, name, -1).astype(f32)
        named = jnp.zeros((pad, total), f32)
        high = jnp.zeros((pad, total), f32)
        low = jnp.zeros((pad, total), f32)
        for k in range(top):
            same = ids[k : k + 1, :] == name
            named = named + jnp.where(same, 1.0, 0.0)
            high = high + jnp.where(same, highs[k : k + 1, :], 0.0)
            low = low + jnp.where(same, lows[k : k + 1, :], 0.0)
        rank = jnp.dot(named.astype(bf16), ahead_ref[...], preferred_element_type=f32)
        rank = jnp.where(named > 0.5, rank, -1.0)
        wanted = wanted_ref[...]
        for j in range(experts):
            hit = rank[j : j + 1, :] == wanted
            at = slice(j * held, (j + 1) * held)
            pick_ref[at, :] = jnp.where(hit, 1.0, 0.0).astype(bf16)
            high_ref[at, :] = jnp.where(hit, high[j : j + 1, :], 0.0).astype(bf16)
            low_ref[at, :] = jnp.where(hit, low[j : j + 1, :], 0.0).astype(bf16)
        sent = jnp.dot(pick_ref[...], own_ref[...], preferred_element_type=f32).astype(bf16)
        for d in range(n_dp):
            out_ref[d] = sent

    slots = experts * held
    outs = (((n_dp, slots, part), bf16),) + (((slots, total), bf16),) * 2
    scratch = [pltpu.VMEM((slots, total), bf16), pltpu.VMEM((total, part), bf16)]
    return call(body, outs, [SMEM] + [VMEM] * 3, scratch)(pair, gathered, ahead, wanted)


def hidden_rows(received, w_gate, w_up):
    n_dp, slots, part = received.shape
    units = w_gate.shape[1]

    def body(rows_ref, gate_ref, up_ref, out_ref):
        half = slots // 2
        for h in range(2):
            here = slice(h * half, (h + 1) * half)
            v = jnp.zeros((half, units), f32)
            u = jnp.zeros((half, units), f32)
            for d in range(n_dp):
                rows = rows_ref[d, here, :]
                at = slice(d * part, (d + 1) * part)
                v = v + jnp.dot(rows, gate_ref[at, :], preferred_element_type=f32)
                u = u + jnp.dot(rows, up_ref[at, :], preferred_element_type=f32)
            made = (v / (1.0 + jnp.exp(-v)) * u).astype(bf16)
            for d in range(n_dp):
                out_ref[d, here, :] = made

    return call(body, [((n_dp, slots, units), bf16)], [VMEM] * 3)(received, w_gate, w_up)


def output_rows(hidden, downs, member):
    n_dp, slots, _ = hidden.shape
    part = downs[0].shape[1]

    def body(member_ref, hidden_ref, *refs):
        out_ref = refs[-1]
        total = jnp.zeros((slots, part), f32)
        for s in range(n_dp):
            source = lax.rem(member_ref[0] + (n_dp - s), n_dp)
            total = total + jnp.dot(hidden_ref[source], refs[s][...], preferred_element_type=f32)
        out_ref[...] = total.astype(bf16)

    return call(body, [((slots, part), bf16)], [SMEM, VMEM] + [VMEM] * n_dp)(
        member, hidden, *downs
    )


def mix_rows(received, high, low, share, n_dp):
    _, part = received.shape
    total = high.shape[1]

    def body(rows_ref, high_ref, low_ref, out_ref):
        rows = rows_ref[...]
        dims = (((0,), (0,)), ((), ()))
        mixed = lax.dot_general(high_ref[...], rows, dims, preferred_element_type=f32)
        mixed = mixed + lax.dot_general(low_ref[...], rows, dims, preferred_element_type=f32)
        for i in range(total // share):
            block, owner = i // n_dp, i % n_dp
            out_ref[owner * (total // share // n_dp) + block] = mixed[i * share : (i + 1) * share, :].astype(bf16)

    return call(body, [((total // share, share, part), bf16)], [VMEM] * 3)(received, high, low)


def sum_rows(shares, n_dp):
    peers, share, part = shares.shape

    def body(shares_ref, out_ref):
        for d in range(n_dp):
            first = d * (peers // n_dp)
            total = shares_ref[first].astype(f32)
            for z in range(1, peers // n_dp):
                total = total + shares_ref[first + z].astype(f32)
            out_ref[:, d * part : (d + 1) * part] = total.astype(bf16)

    return call(body, [((share, n_dp * part), bf16)], [VMEM])(shares)


def exchange(value, axes):
    return lax.all_to_all(value, axes, split_axis=0, concat_axis=0, tiled=True)


def on_device(tokens, expert_ids, route_logits, expert_gate, expert_up, expert_down):
    rows, width = tokens.shape
    top = expert_ids.shape[1]
    n_x, n_pair, n_c, n_dp = (lax.axis_size(a) for a in ("x", "zh", "c", "y"))
    part = width // n_dp
    experts = n_x * 2 * n_c
    held = n_pair * SLOTS
    slots = experts * held
    member = lax.axis_index("y").astype(i32)
    member_ref = member.reshape(1)
    pair_ref = lax.axis_index("zh").astype(i32).reshape(1)
    w_gate, w_up = expert_gate[0], expert_up[0]

    packed = pack_rows(tokens, expert_ids, route_logits, member_ref, n_dp, n_pair)
    gathered = exchange(packed, "zh")

    downs = []
    for s in range(n_dp):
        owner = member + s
        owner = jnp.where(owner >= n_dp, owner - n_dp, owner)
        piece = lax.dynamic_slice_in_dim(expert_down[0], owner * part, part, axis=1)
        if s:
            piece = lax.ppermute(piece, "y", [(i, (i + s) % n_dp) for i in range(n_dp)])
        downs.append(piece)

    ahead, wanted = route_masks(pair_ref, n_pair * rows, rows, held)
    outgoing, high, low = route_rows(
        gathered, pair_ref, ahead, wanted, rows, top, n_x, n_pair, n_c, n_dp
    )
    arrived = exchange(outgoing.reshape(n_dp * experts, held, part), ("y", "c", "x", "zl"))
    hidden = hidden_rows(arrived.reshape(n_dp, slots, part), w_gate, w_up)
    hidden, downs = lax.optimization_barrier((hidden, downs))
    hidden = exchange(hidden, "y")
    results = output_rows(hidden, downs, member_ref)
    back = exchange(results.reshape(experts, held, part), ("c", "x", "zl"))
    mixed = mix_rows(back.reshape(slots, part), high, low, rows // n_dp, n_dp)
    shares = exchange(mixed, ("y", "zh"))
    return sum_rows(shares, n_dp)


def solution(mesh):
    n_ep, n_dp = mesh.devices.shape
    grid = mesh.devices.reshape(CHIPS_X, n_ep // (CHIPS_X * 2 * CORES), 2, CORES, n_dp)
    fine = Mesh(grid, ("x", "zh", "zl", "c", "y"))
    ep = ("x", "zh", "zl", "c")
    placed = (
        P(ep, None),
        P(ep, None),
        P(ep, None),
        P(ep, None, "y"),
        P(ep, None, "y"),
        P(ep, "y", None),
    )
    return jax.shard_map(
        on_device, mesh=fine, in_specs=placed, out_specs=P(ep + ("y",), None), check_vma=False
    )
```
